32 devices in a mesh: cells: 8 (over y, x, core), genes: 4 (over z).
Axes of the slice: x: 2, y: 2, z: 4, core: 2. Of those that a mesh axis runs over, the one named last changes fastest.
Arguments:
- counts: int32 [8192, 4096], P('cells', 'genes'), may hold values from 0 to 26, as said below
- library: int32 [8192], P('cells'), may hold values from 2000 to 19999
Outputs:
- adjacency: float32 [4096, 4096], P('cells', 'genes')
- connectivity: float32 [4096], P('cells')
The draws below stay inside these ranges and needn't reach their ends.
Inputs may be any that keep to these rules, and one draw needn't show every extreme that they name: Non-negative integer counts.
All inputs are finite; a program needn't handle non-finite values.
Results may differ from the reference program's by a relative error of at most 0.006.
Values may be sent and summed in bfloat16 or wider, within the bound.
No kernel may reach another device: no remote copies, remote signals or barrier semaphores. Data moves between devices by JAX's collectives and lax.ppermute only.
A program may use at most 128 MiB of HBM per device.

```python
import jax
import jax.numpy as jnp
from jax import lax

G = 4096
CELLS_DEV = 1024
CELLS = 8192
N_CELLS = 8


module_count = 32


def draw_counts(key, part):
    module_ids = jax.random.randint(jax.random.fold_in(key, 11), (G,), 0, module_count)
    levels = jax.random.randint(jax.random.fold_in(key, 12), (CELLS, module_count), 0, 8)
    gains = jax.random.randint(jax.random.fold_in(key, 13), (G,), 0, 4)
    noise = jax.random.randint(jax.random.fold_in(key, 14), (CELLS, G), 0, 6)
    present = jax.random.randint(jax.random.fold_in(key, 15), (CELLS, G), 0, 3)
    shared = jnp.take(levels, module_ids, axis=1)
    values = noise + gains[None, :] * shared
    return jnp.where(present > 0, values, 0).astype(jnp.int32)


def place_ends(values, rng, low, high):
    longest = values.shape.index(max(values.shape))
    spots = []
    for shift in (0, 1):
        where = [jax.random.randint(jax.random.fold_in(rng, axis), (), 0, length) for axis, length in enumerate(values.shape)]
        where[longest] = (where[longest] + shift) % values.shape[longest]
        spots.append(tuple(where))
    return values.at[spots[0]].set(low).at[spots[1]].set(high)


def setup_inputs(seed: int = 0) -> dict:
    splits = jax.random.split(jax.random.key(seed), 3)
    return {
        "counts": draw_counts(jax.random.fold_in(splits[2], 71), 0),
        "library": place_ends(jax.random.randint(splits[1], (CELLS,), 2000, 20000), jax.random.fold_in(splits[1], 1), 2000, 19999).astype(jnp.int32),
    }


def normalize(counts, library):
    factor = 10000.0 / library.astype(jnp.float32)
    return jnp.log1p(counts.astype(jnp.float32) * factor[:, None]).astype(jnp.bfloat16)

def reference(counts, library):
    count_blocks = counts.reshape(N_CELLS, CELLS_DEV, G)
    library_blocks = library.reshape(N_CELLS, CELLS_DEV)

    def accumulate(carry, inputs):
        gram, sums, squares = carry
        expressed = normalize(inputs[0], inputs[1]).astype(jnp.float32)
        gram = gram + jnp.dot(expressed.T, expressed, precision=lax.Precision.HIGHEST, preferred_element_type=jnp.float32)
        sums = sums + lax.optimization_barrier(jnp.sum(expressed, axis=0))
        squares = squares + lax.optimization_barrier(jnp.sum(expressed * expressed, axis=0))
        return ((gram, sums, squares), None)
    start = (jnp.zeros((G, G), jnp.float32), jnp.zeros((G,), jnp.float32), jnp.zeros((G,), jnp.float32))
    (gram, sums, squares), unused = lax.scan(accumulate, start, (count_blocks, library_blocks))
    total_cells = float(CELLS)
    means = sums / total_cells
    variances = squares / total_cells - means * means
    scales = lax.rsqrt(variances + 1e-05)
    correlation = (gram / total_cells - means[:, None] * means[None, :]) * scales[:, None] * scales[None, :]
    powered = correlation ** 6
    diagonal = jnp.arange(G)[:, None] == jnp.arange(G)[None, :]
    adjacency = jnp.where(diagonal, jnp.float32(0.0), powered)
    connectivity = lax.optimization_barrier(jnp.sum(adjacency, axis=1))
    return (adjacency, connectivity)
```

```python
import functools

import jax
import jax.numpy as jnp
from jax import lax
from jax.experimental import pallas as pl
from jax.experimental.pallas import tpu as pltpu
from jax.sharding import PartitionSpec as P


AXES = ("cells", "genes")


def normalize(counts, library):
    factor = 10000.0 / library.astype(jnp.float32)
    return jnp.log1p(counts.astype(jnp.float32) * factor[:, None]).astype(jnp.bfloat16)


def cross_product(left, right):
    return lax.dot_general(
        left, right, (((0,), (0,)), ((), ())), preferred_element_type=jnp.float32
    )


def general_shards(counts, library):
    own_block = normalize(counts, library)
    col_width = own_block.shape[1]
    cell_groups = lax.axis_size("cells")
    gene_total = col_width * lax.axis_size("genes")
    row_width = gene_total // cell_groups
    total_cells = float(counts.shape[0] * cell_groups)
    widened = own_block.astype(jnp.float32)
    local_sums = jnp.sum(widened, axis=0)
    local_squares = jnp.sum(widened * widened, axis=0)
    block_sums, block_squares = lax.psum((local_sums, local_squares), "cells")
    gene_sums, gene_squares = (
        lax.all_gather(block_sums, "genes", axis=0, tiled=True),
        lax.all_gather(block_squares, "genes", axis=0, tiled=True),
    )
    full_block = lax.all_gather(own_block, "genes", axis=1, tiled=True)
    gram_tile = lax.psum_scatter(
        cross_product(full_block, own_block), "cells", scatter_dimension=0, tiled=True
    )
    means = gene_sums / total_cells
    variances = gene_squares / total_cells - means * means
    scales = lax.rsqrt(variances + 1e-05)
    row_first = lax.axis_index("cells") * row_width
    col_first = lax.axis_index("genes") * col_width
    row_means = lax.dynamic_slice_in_dim(means, row_first, row_width, 0)
    col_means = lax.dynamic_slice_in_dim(means, col_first, col_width, 0)
    row_scales = lax.dynamic_slice_in_dim(scales, row_first, row_width, 0)
    col_scales = lax.dynamic_slice_in_dim(scales, col_first, col_width, 0)
    correlation = (
        (gram_tile / total_cells - row_means[:, None] * col_means[None, :])
        * row_scales[:, None]
        * col_scales[None, :]
    )
    powered = correlation**6
    row_index = row_first + jnp.arange(row_width, dtype=jnp.int32)[:, None]
    col_index = col_first + jnp.arange(col_width, dtype=jnp.int32)[None, :]
    adjacency = jnp.where(row_index == col_index, jnp.float32(0.0), powered)
    connectivity = lax.psum(jnp.sum(adjacency, axis=1), "genes")
    return (adjacency, connectivity)


def encode(x):
    x2 = x * x
    return (x2 * x2 * x).astype(jnp.bfloat16)


def decode(y):
    y = y.astype(jnp.float32)
    root = jnp.exp2(jnp.log2(jnp.abs(y)) * 0.2)
    return jnp.where(y < 0, -root, root)


def block_body(s_ref, x0, x1, y0, y1, rst, cst, own_ref, send_ref, acc, sxa, sya, *, n_s, cells, total):
    s = pl.program_id(1)
    jj = pl.program_id(0)
    ones_r = jnp.ones((x0.shape[-2], 128), jnp.bfloat16)
    ones_l = jnp.ones((8, x0.shape[-2]), jnp.bfloat16)
    a0, a1 = x0[...].reshape(x0.shape[-2:]), x1[...].reshape(x1.shape[-2:])
    b0, b1 = y0[...].reshape(y0.shape[-2:]), y1[...].reshape(y1.shape[-2:])
    part = cross_product(a0, b0) + cross_product(a1, b1)
    sx = cross_product(a0, ones_r) + cross_product(a1, ones_r)
    sy = jnp.dot(ones_l, b0, preferred_element_type=jnp.float32) + jnp.dot(
        ones_l, b1, preferred_element_type=jnp.float32
    )
    if n_s > 1:

        @pl.when(s == 0)
        def _():
            acc[...] = part
            sxa[...] = sx
            sya[...] = sy

        @pl.when(s > 0)
        def _():
            acc[...] += part
            sxa[...] += sx
            sya[...] += sy

    else:
        acc[...] = part
        sxa[...] = sx
        sya[...] = sy

    @pl.when(s == n_s - 1)
    def _():
        col_side = cst[0]
        row_side = rst[0].T
        mc, sc = col_side[0:1], col_side[1:2]
        mr, sr = row_side[:, 0:1], row_side[:, 1:2]
        rest = sya[0:1, :] - cells * mc
        p = acc[...] - sxa[:, 0:1] * mc - mr * rest
        p = p * (sr * (1.0 / total)) * sc
        odd = s_ref[0] % 2
        t = p.shape[0] // 2
        tiles = [[p[i * t : i * t + t, c * t : c * t + t] for c in range(2)] for i in range(2)]
        for b in range(2):
            for i in range(2):
                tile = jnp.where(odd == 0, tiles[i][i ^ b], tiles[i][1 - (i ^ b)])
                send_ref[b, i] = encode(tile)
                if b == 0:

                    @pl.when(jj == 0)
                    def _():
                        own_ref[i] = tile


def block_call(scal, x0, x1, y0, y1, stats, x_maps, y_maps, n_s, half_cells, half, tile, total):
    def row_map(jj, s, sc):
        return (sc[2], 0, sc[1])

    def col_map(jj, s, sc):
        return (sc[3], 0, sc[1] ^ (sc[0] // 2) ^ jj)

    def spec(arr, m):
        lead = arr.ndim - 2
        return pl.BlockSpec((1,) * lead + (half_cells, half), m)

    body = functools.partial(block_body, n_s=n_s, cells=float(2 * half_cells * n_s), total=total)
    return pl.pallas_call(
        body,
        grid_spec=pltpu.PrefetchScalarGridSpec(
            num_scalar_prefetch=1,
            grid=(2, n_s),
            in_specs=[
                spec(x0, x_maps[0]),
                spec(x1, x_maps[1]),
                spec(y0, y_maps[0]),
                spec(y1, y_maps[1]),
                pl.BlockSpec((1, 8, half), row_map),
                pl.BlockSpec((1, 8, half), col_map),
            ],
            out_specs=[
                pl.BlockSpec((2, tile, tile), lambda jj, s, sc: (0, 0, 0)),
                pl.BlockSpec((2, 2, tile, tile), lambda jj, s, sc: (jj, 0, 0, 0)),
            ],
            scratch_shapes=[
                pltpu.VMEM((half, half), jnp.float32),
                pltpu.VMEM((half, 128), jnp.float32),
                pltpu.VMEM((8, half), jnp.float32),
            ],
        ),
        out_shape=[
            jax.ShapeDtypeStruct((2, tile, tile), jnp.float32),
            jax.ShapeDtypeStruct((4, 2, tile, tile), jnp.bfloat16),
        ],
        name="partial_block",
    )(scal, x0, x1, y0, y1, stats, stats)


def place_body(s_ref, t0, t1, t2, t3, out_ref, sum_ref):
    x = s_ref[0]
    tiles = (t0, t1, t2, t3)
    t = t0.shape[-1]
    for i in range(2):
        total = jnp.zeros((t, 1), jnp.float32)
        for c in range(4):
            v = tiles[c ^ i][i].astype(jnp.float32)
            for m in range(1, 4):
                v = jnp.where(x == m, tiles[c ^ i ^ m][i].astype(jnp.float32), v)
            out_ref[i * t : i * t + t, c * t : c * t + t] = v
            total = total + jnp.sum(v, axis=1, keepdims=True)
        sum_ref[i * t : i * t + t, :] = total


def folded_shards(counts, library):
    rows, width = counts.shape
    n_cells = lax.axis_size("cells")
    n_genes = lax.axis_size("genes")
    cores = n_cells // n_genes
    total = float(rows * n_cells)
    half_cells = rows // 2
    half = width // cores
    tile = half // 2
    g = lax.axis_index("genes")
    c = lax.axis_index("cells")
    k, h = c // cores, c % cores

    def perm(f):
        pairs = []
        for ci in range(n_cells):
            for gi in range(n_genes):
                d = f(ci // cores, ci % cores, gi)
                if d is not None and 0 <= d[2] < n_genes:
                    pairs.append((ci * n_genes + gi, (d[0] * cores + d[1]) * n_genes + d[2]))
        return pairs

    def send(x, f):
        return lax.ppermute(x, AXES, perm(f))

    up = lambda k, h, g: (k, h, g + 1)
    down = lambda k, h, g: (k, h, g - 1)
    flip = lambda k, h, g: (k, h ^ 1, g)

    own = normalize(counts, library)
    oth = send(own, flip)
    widened = own.astype(jnp.float32)
    local = jnp.stack([jnp.sum(widened, axis=0), jnp.sum(widened * widened, axis=0)])
    slots = jnp.where(jnp.arange(n_genes)[:, None, None] == g, local[None], 0.0)
    sums = lax.psum(slots, AXES)
    means = sums[:, 0] / total
    variances = sums[:, 1] / total - means * means
    scales = lax.rsqrt(variances + 1e-05)
    stats = jnp.pad(jnp.stack([means, scales], axis=1), ((0, 0), (0, 6), (0, 0)))

    def payload(first):
        return jnp.stack(
            [lax.dynamic_slice(a, (first, h * half), (half_cells, half)) for a in (own, oth)]
        )

    pay_a = payload(0)
    pay_b = payload(half_cells)
    up1 = send(pay_a, up)
    dn1 = send(pay_b, down)
    up2 = send(jnp.where(g == 0, pay_b, up1), up)
    dn2 = send(jnp.where(g == n_genes - 1, pay_a, dn1), down)
    upper = g >= n_genes // 2
    far = jnp.where(upper, up2, dn2)
    near = jnp.where(upper, dn2, up2)
    near_other = send(near, flip)
    both = jnp.concatenate([near, near_other])

    def scal(q, p, s):
        return jnp.stack([k, h, q, p, s]).astype(jnp.int32)

    col = lambda jj, sc: sc[1] ^ (sc[0] // 2) ^ jj
    x_own = lambda jj, s, sc: (s, sc[1])
    y_own = lambda jj, s, sc: (s, col(jj, sc))
    x_part = [lambda jj, s, sc, p=p: (p, 0, 0) for p in (0, 1)]
    y_half = lambda jj, s, sc: (sc[4], col(jj, sc))

    def y_both(p):
        def m(jj, s, sc):
            d = (sc[0] // 2) ^ jj
            return (2 * d + (p ^ d), 0, 0)

        return m

    call = functools.partial(block_call, stats=stats, half_cells=half_cells, half=half, tile=tile, total=total)
    clip = lambda q: jnp.clip(q, 0, n_genes - 1)
    w0 = call(scal(g, g, 0), own, oth, own, oth, x_maps=(x_own, x_own), y_maps=(y_own, y_own), n_s=2)
    wu = call(scal(clip(g - 1), g, 0), up1, up1, own, oth, x_maps=x_part, y_maps=(y_half, y_half), n_s=1)
    wd = call(scal(clip(g + 1), g, 1), dn1, dn1, own, oth, x_maps=x_part, y_maps=(y_half, y_half), n_s=1)
    q2 = g ^ 2
    w2 = call(
        scal(q2, g, jnp.where(upper, 0, 1)), far, far, own, oth, x_maps=x_part, y_maps=(y_half, y_half), n_s=1
    )
    w3 = call(
        scal(q2, g ^ 1, 0), far, far, both, both, x_maps=x_part, y_maps=(y_both(0), y_both(1)), n_s=1
    )

    def reduce_tiles(blocks):
        parts = []
        for j in range(1, 4):
            msg = jnp.stack([b[1][j] for b in blocks])
            parts.append(send(msg, lambda k, h, g, j=j: (k ^ j, h, g)))
        return [
            b[0] + decode(parts[0][n]) + decode(parts[1][n]) + decode(parts[2][n])
            for n, b in enumerate(blocks)
        ]

    (t0,) = reduce_tiles([w0])
    tu, td = reduce_tiles([wu, wd])
    t2, t3 = reduce_tiles([w2, w3])

    def turned(t):
        e = jnp.swapaxes(encode(t), 1, 2)
        return jnp.where(k % 2 == 0, e, e[::-1])

    side = lambda f: (lambda k, h, g: (k, h ^ (k // 2), f(g)) if f(g) is not None else None)
    ru = send(turned(td), side(lambda g: g + 1))
    rd = send(turned(tu), side(lambda g: g - 1))
    r2 = send(turned(t2), side(lambda g: g ^ 2))
    r3f = send(turned(t3), side(lambda g: {1: 3, 2: 0}.get(g)))
    r3n = send(encode(t3), lambda k, h, g: (k, h, {1: 0, 2: 3}[g]) if g in (1, 2) else None)

    def power(v):
        v2 = v * v
        return (v2 * v2 * v2).astype(jnp.bfloat16)

    rr = 2 * h + jnp.arange(2)
    same_tile = (rr == (rr ^ k))[:, None, None]
    eye = jnp.eye(tile, dtype=bool)[None]
    a0 = jnp.where(same_tile & eye, 0.0, power(t0).astype(jnp.float32)).astype(jnp.bfloat16)
    au = power(tu + decode(ru))
    ad = power(td + decode(rd))
    a2 = power(t2 + decode(r2))
    a3 = power(decode(r3n) + decode(r3f))

    early = jnp.stack([au, a0, ad])
    late = jnp.stack([a2, a3])
    is_early = lambda q, g: -1 <= q - g <= 1

    def pick_early(q):
        return lax.dynamic_index_in_dim(early, jnp.clip(q - g + 1, 0, 2), 0, keepdims=False)

    def pick_late(q):
        return lax.dynamic_index_in_dim(late, jnp.where((q ^ g) == 2, 0, 1), 0, keepdims=False)

    mine_early = jnp.abs(k - g) <= 1
    placed = [jnp.where(mine_early, pick_early(k), pick_late(k))]
    for j in range(1, 4):
        e = send(
            pick_early(k ^ j), lambda k, h, g, j=j: (k ^ j, h, g) if is_early(k ^ j, g) else None
        )
        l = send(
            pick_late(k ^ j), lambda k, h, g, j=j: (k ^ j, h, g) if not is_early(k ^ j, g) else None
        )
        placed.append(jnp.where(mine_early, e, l))

    full = pl.BlockSpec(memory_space=pltpu.VMEM)
    adjacency, row_sums = pl.pallas_call(
        place_body,
        in_specs=[pl.BlockSpec(memory_space=pltpu.SMEM)] + [full] * 4,
        out_specs=[full, full],
        out_shape=[
            jax.ShapeDtypeStruct((half, width), jnp.float32),
            jax.ShapeDtypeStruct((half, 1), jnp.float32),
        ],
        name="place_tiles",
    )(((2 * h) ^ k).reshape(1).astype(jnp.int32), *placed)
    part = row_sums[:, 0]
    near_sum = [send(part, lambda k, h, g, d=d: (k, h, g ^ d)) for d in (1, 2, 3)]
    connectivity = (part + near_sum[0]) + (near_sum[1] + near_sum[2])
    return (adjacency, connectivity)


def solution(mesh):
    cells, genes = mesh.shape["cells"], mesh.shape["genes"]
    folds = genes == 4 and cells == 2 * genes
    return jax.shard_map(
        folded_shards if folds else general_shards,
        mesh=mesh,
        in_specs=(P("cells", "genes"), P("cells")),
        out_specs=(P("cells", "genes"), P("cells")),
        check_vma=False,
    )
```

```python
import functools

import jax
import jax.numpy as jnp
from jax import lax
from jax.experimental import pallas as pl
from jax.experimental.pallas import tpu as pltpu
from jax.sharding import PartitionSpec as P


AXES = ("cells", "genes")


def normalize(counts, library):
    factor = 10000.0 / library.astype(jnp.float32)
    return jnp.log1p(counts.astype(jnp.float32) * factor[:, None]).astype(jnp.bfloat16)


def cross_product(left, right):
    return lax.dot_general(
        left, right, (((0,), (0,)), ((), ())), preferred_element_type=jnp.float32
    )


def general_shards(counts, library):
    own_block = normalize(counts, library)
    col_width = own_block.shape[1]
    cell_groups = lax.axis_size("cells")
    gene_total = col_width * lax.axis_size("genes")
    row_width = gene_total // cell_groups
    total_cells = float(counts.shape[0] * cell_groups)
    widened = own_block.astype(jnp.float32)
    local_sums = jnp.sum(widened, axis=0)
    local_squares = jnp.sum(widened * widened, axis=0)
    block_sums, block_squares = lax.psum((local_sums, local_squares), "cells")
    gene_sums, gene_squares = (
        lax.all_gather(block_sums, "genes", axis=0, tiled=True),
        lax.all_gather(block_squares, "genes", axis=0, tiled=True),
    )
    full_block = lax.all_gather(own_block, "genes", axis=1, tiled=True)
    gram_tile = lax.psum_scatter(
        cross_product(full_block, own_block), "cells", scatter_dimension=0, tiled=True
    )
    means = gene_sums / total_cells
    variances = gene_squares / total_cells - means * means
    scales = lax.rsqrt(variances + 1e-05)
    row_first = lax.axis_index("cells") * row_width
    col_first = lax.axis_index("genes") * col_width
    row_means = lax.dynamic_slice_in_dim(means, row_first, row_width, 0)
    col_means = lax.dynamic_slice_in_dim(means, col_first, col_width, 0)
    row_scales = lax.dynamic_slice_in_dim(scales, row_first, row_width, 0)
    col_scales = lax.dynamic_slice_in_dim(scales, col_first, col_width, 0)
    correlation = (
        (gram_tile / total_cells - row_means[:, None] * col_means[None, :])
        * row_scales[:, None]
        * col_scales[None, :]
    )
    powered = correlation**6
    row_index = row_first + jnp.arange(row_width, dtype=jnp.int32)[:, None]
    col_index = col_first + jnp.arange(col_width, dtype=jnp.int32)[None, :]
    adjacency = jnp.where(row_index == col_index, jnp.float32(0.0), powered)
    connectivity = lax.psum(jnp.sum(adjacency, axis=1), "genes")
    return (adjacency, connectivity)


def encode(x):
    x2 = x * x
    return (x2 * x2 * x).astype(jnp.bfloat16)


def decode(y):
    y = y.astype(jnp.float32)
    root = jnp.exp2(jnp.log2(jnp.abs(y)) * 0.2)
    return jnp.where(y < 0, -root, root)


def block_tiles(p, odd):
    t = p.shape[0] // 2
    tiles = [[p[i * t : i * t + t, c * t : c * t + t] for c in range(2)] for i in range(2)]
    return [
        [jnp.where(odd == 0, tiles[i][i ^ b], tiles[i][1 - (i ^ b)]) for i in range(2)]
        for b in range(2)
    ]


def centred(p, sx, sy, rst, cst, cells, total):
    mc, sc = cst[0:1], cst[1:2]
    row_side = rst.T
    mr, sr = row_side[:, 0:1], row_side[:, 1:2]
    p = p - sx[:, 0:1] * mc - mr * (sy[0:1] - cells * mc)
    return p * (sr * (1.0 / total)) * sc


def plain(left, right):
    return jnp.dot(left, right, preferred_element_type=jnp.float32)


def against_rows(left, right):
    return lax.dot_general(
        left, right, (((1,), (1,)), ((), ())), preferred_element_type=jnp.float32
    )


def put_tiles(p, s_ref, jj, blk, own_ref, sends):
    tiles = block_tiles(p, s_ref[0] % 2)
    for b in range(2):
        for i in range(2):

            @pl.when(jj == 0)
            def _():
                if b == 0:
                    own_ref[blk, i] = tiles[b][i]
                else:
                    sends[0][blk, i] = encode(tiles[b][i])

            @pl.when(jj == 1)
            def _():
                sends[1 + b][blk, i] = encode(tiles[b][i])


def local_products(x, y0, y1):
    n = y0.shape[0]
    right = jnp.ones((x.shape[1], 128), jnp.bfloat16)
    left = jnp.ones((8, n), jnp.bfloat16)
    p = plain(x[:, :n], y0) + plain(x[:, n:], y1)
    return p, plain(x, right), plain(left, y0) + plain(left, y1)


def diagonal_body(s_ref, xa, xb, y0, y1, rst, cst, own_ref, o1, o2, o3, acc, sxa, sya, *, total):
    jj, s = pl.program_id(0), pl.program_id(1)
    n_s = pl.num_programs(1)
    x = jnp.where(s == 0, xa[...], xb[...])
    p, sx, sy = local_products(x, y0[...], y1[...])

    @pl.when(s == 0)
    def _():
        acc[...] = p
        sxa[...] = sx
        sya[...] = sy

    @pl.when(s > 0)
    def _():
        acc[...] += p
        sxa[...] += sx
        sya[...] += sy

    @pl.when(s == n_s - 1)
    def _():
        cells = 4.0 * y0.shape[0]
        p = centred(acc[...], sxa[...], sya[...], rst[0], cst[0], cells, total)
        put_tiles(p, s_ref, jj, 0, own_ref, (o1, o2, o3))


def near_body(s_ref, xa, xb, y0, y1, rst, cst, own_ref, o1, o2, o3, *, total):
    blk, jj = pl.program_id(0), pl.program_id(1)
    x = jnp.where(blk == 0, xa[...], xb[...])
    p, sx, sy = local_products(x, y0[...], y1[...])
    p = centred(p, sx, sy, rst[0], cst[0], 2.0 * y0.shape[0], total)
    put_tiles(p, s_ref, jj, blk, own_ref, (o1, o2, o3))


def far_body(s_ref, xa, xb, y0, y1, na, nb, rst, cst, own_ref, o1, o2, o3, acc, sya, *, total):
    blk, jj = pl.program_id(0), pl.program_id(1)
    x = jnp.where(s_ref[2] == 0, xa[...], xb[...])
    n = y0.shape[0]
    left = jnp.ones((8, 2 * n), jnp.bfloat16)
    right = jnp.ones((2 * n, 128), jnp.bfloat16)
    sx = plain(x, right)

    @pl.when(blk == 0)
    def _():
        acc[...] = plain(x[:, :n], y0[...]) + plain(x[:, n:], y1[...])
        sya[...] = plain(left[:, :n], y0[...]) + plain(left[:, n:], y1[...])

    other = (s_ref[0] // 2) ^ jj

    @pl.when((blk == 1) & (other == 0))
    def _():
        acc[...] = against_rows(x, na[...])
        sya[...] = against_rows(left, na[...])

    @pl.when((blk == 1) & (other == 1))
    def _():
        acc[...] = against_rows(x[:, :n], nb[:, n:]) + against_rows(x[:, n:], nb[:, :n])
        sya[...] = against_rows(left, nb[...])

    p = centred(acc[...], sx, sya[...], rst[0], cst[0], 2.0 * n, total)
    put_tiles(p, s_ref, jj, blk, own_ref, (o1, o2, o3))


def turn_body(s_ref, own, r1, r2, r3, *outs, turns, keeps):
    odd = s_ref[0] % 2
    t_ref, rest = outs[0], outs[1:]
    for n in range(own.shape[0]):
        for i in range(2):
            v = own[n, i] + decode(r1[n, i]) + decode(r2[n, i]) + decode(r3[n, i])
            t_ref[n, i] = v
            if keeps[n] is not None:
                rest[keeps[n]][i] = encode(v)
            if turns[n] is not None:
                w = encode(v.T)
                dst = rest[turns[n]]

                @pl.when(odd == 0)
                def _():
                    dst[i] = w

                @pl.when(odd == 1)
                def _():
                    dst[1 - i] = w


def power(v):
    v2 = v * v
    return v2 * v2 * v2


def put_slot(outs, where, i, value):
    for j, o in enumerate(outs):

        @pl.when(where == j)
        def _():
            o[i] = value


def early_body(s_ref, t0, t1, ru, rd, *outs):
    k, g = s_ref[0], s_ref[2]
    n = t0.shape[-1]
    for i in range(2):
        own = power(t0[0, i])
        same = lax.broadcasted_iota(jnp.int32, (n, n), 0) == lax.broadcasted_iota(
            jnp.int32, (n, n), 1
        )
        own = jnp.where(same & (k == 0), 0.0, own).astype(jnp.bfloat16)
        put_slot(outs, g ^ k, i, own)
        low = power(t1[0, i] + decode(ru[i])).astype(jnp.bfloat16)
        put_slot(outs, jnp.where(g > 0, (g - 1) ^ k, -1), i, low)
        high = power(t1[1, i] + decode(rd[i])).astype(jnp.bfloat16)
        put_slot(outs, jnp.where(g < s_ref[3] - 1, (g + 1) ^ k, -1), i, high)


def late_body(s_ref, t2, r2, rf, rn, *outs):
    k, g = s_ref[0], s_ref[2]
    outer = (g == 0) | (g == s_ref[3] - 1)
    for i in range(2):
        two = power(t2[0, i] + decode(r2[i])).astype(jnp.bfloat16)
        put_slot(outs, g ^ 2 ^ k, i, two)
        three = power(decode(rf[i]) + decode(rn[i])).astype(jnp.bfloat16)
        put_slot(outs, jnp.where(outer, g ^ 3 ^ k, -1), i, three)


def place_body(s_ref, e0, e1, e2, e3, l0, l1, l2, l3, out_ref, sum_ref):
    x = s_ref[0]
    is_early = s_ref[1]
    early, late = (e0, e1, e2, e3), (l0, l1, l2, l3)
    t = e0.shape[-1]

    def place(tiles):
        for i in range(2):
            total = jnp.zeros((t, 1), jnp.float32)
            for c in range(4):
                v = tiles[c ^ i][i]
                for m in range(1, 4):
                    v = jnp.where(x == m, tiles[c ^ i ^ m][i], v)
                v = v.astype(jnp.float32)
                out_ref[i * t : i * t + t, c * t : c * t + t] = v
                total = total + jnp.sum(v, axis=1, keepdims=True)
            sum_ref[i * t : i * t + t, :] = total

    @pl.when(is_early == 1)
    def _():
        place(early)

    @pl.when(is_early == 0)
    def _():
        place(late)


def pay_body(s_ref, a, b, out_a, out_b):
    n = a.shape[0]
    for s, out in enumerate((out_a, out_b)):

        @pl.when(pl.program_id(0) == s)
        def _():
            out[:, :n] = a[...].T
            out[:, n:] = b[...].T


def whole():
    return pl.BlockSpec(memory_space=pltpu.VMEM)


def scalars():
    return pl.BlockSpec(memory_space=pltpu.SMEM)


def folded_shards(counts, library):
    rows, width = counts.shape
    n_cells = lax.axis_size("cells")
    n_genes = lax.axis_size("genes")
    cores = n_cells // n_genes
    total = float(rows * n_cells)
    half_cells = rows // 2
    half = width // cores
    tile = half // 2
    g = lax.axis_index("genes")
    c = lax.axis_index("cells")
    k, h = c // cores, c % cores

    def perm(f):
        pairs = []
        for ci in range(n_cells):
            for gi in range(n_genes):
                d = f(ci // cores, ci % cores, gi)
                if d is not None and 0 <= d[2] < n_genes:
                    pairs.append((ci * n_genes + gi, (d[0] * cores + d[1]) * n_genes + d[2]))
        return pairs

    def send(x, f):
        return lax.ppermute(x, AXES, perm(f))

    flip = lambda k, h, g: (k, h ^ 1, g)
    bf16, f32 = jnp.bfloat16, jnp.float32
    shape = jax.ShapeDtypeStruct

    own = normalize(counts, library)
    oth = send(own, flip)
    where = jnp.stack([k, h, g, jnp.int32(n_genes)]).astype(jnp.int32)
    pay_a, pay_b = pl.pallas_call(
        pay_body,
        grid_spec=pltpu.PrefetchScalarGridSpec(
            num_scalar_prefetch=1,
            grid=(2,),
            in_specs=[pl.BlockSpec((half_cells, half), lambda s, sc: (s, sc[1]))] * 2,
            out_specs=[pl.BlockSpec((half, 2 * half_cells), lambda s, sc: (0, 0))] * 2,
        ),
        out_shape=[shape((half, 2 * half_cells), bf16)] * 2,
        name="turn_payload",
    )(where, own, oth)
    up1 = send(pay_a, lambda k, h, g: (k, h, g + 1))
    dn1 = send(pay_b, lambda k, h, g: (k, h, g - 1))
    end = jnp.where(g == 0, pay_b, pay_a)
    last = n_genes - 1
    near = send(
        end, lambda k, h, g: (k, h, 1) if g == 0 else ((k, h, g - 1) if g == last else None)
    )
    widened = own.astype(f32)
    local = jnp.stack([jnp.sum(widened, axis=0), jnp.sum(widened * widened, axis=0)])
    sums = lax.psum(local, "cells")
    means = sums[0] / total
    variances = sums[1] / total - means * means
    mine = jnp.stack([means, lax.rsqrt(variances + 1e-05)])
    afar = [send(mine, lambda k, h, g, d=d: (k, h, g ^ d)) for d in (1, 2, 3)]
    widen = ((0, 0), (0, 6), (0, 0))
    own_stats = jnp.pad(mine[None], widen)
    stats = jnp.pad(jnp.stack([mine] + afar), widen)

    def block_outs(n, m):
        spec = pl.BlockSpec((n, 2, tile, tile), m)
        return [spec] * 4

    def out_shapes(n):
        return [shape((n, 2, tile, tile), f32)] + [shape((n, 2, tile, tile), bf16)] * 3

    col = lambda jj, sc: sc[1] ^ (sc[0] // 2) ^ jj
    y_spec = pl.BlockSpec((half_cells, half), lambda jj, s, sc: (s, col(jj, sc)))
    w0 = pl.pallas_call(
        functools.partial(diagonal_body, total=total),
        grid_spec=pltpu.PrefetchScalarGridSpec(
            num_scalar_prefetch=1,
            grid=(2, 2),
            in_specs=[
                pl.BlockSpec((half, 2 * half_cells), lambda jj, s, sc: (0, 0)),
                pl.BlockSpec((half, 2 * half_cells), lambda jj, s, sc: (0, 0)),
                y_spec,
                y_spec,
                pl.BlockSpec((1, 8, half), lambda jj, s, sc: (0, 0, sc[1])),
                pl.BlockSpec((1, 8, half), lambda jj, s, sc: (0, 0, col(jj, sc))),
            ],
            out_specs=block_outs(1, lambda jj, s, sc: (0, 0, 0, 0)),
            scratch_shapes=[
                pltpu.VMEM((half, half), f32),
                pltpu.VMEM((half, 128), f32),
                pltpu.VMEM((8, half), f32),
            ],
        ),
        out_shape=out_shapes(1),
        name="diagonal_block",
    )(where, pay_a, pay_b, own, oth, own_stats, own_stats)

    up2 = send(up1, lambda k, h, g: (k, h, g + 1) if g > 0 else None)
    dn2 = send(dn1, lambda k, h, g: (k, h, g - 1) if g < last else None)
    near_other = send(near, flip)

    x_spec = pl.BlockSpec((half, 2 * half_cells), lambda b, jj, sc: (0, 0))
    lower = jnp.where(g > 0, g ^ (g - 1), 0)
    higher = jnp.where(g < last, g ^ (g + 1), 0)
    scal1 = jnp.stack([k, h, lower, higher]).astype(jnp.int32)
    y_spec = pl.BlockSpec((half_cells, half), lambda b, jj, sc: (b, col(jj, sc)))
    w1 = pl.pallas_call(
        functools.partial(near_body, total=total),
        grid_spec=pltpu.PrefetchScalarGridSpec(
            num_scalar_prefetch=1,
            grid=(2, 2),
            in_specs=[
                x_spec,
                x_spec,
                y_spec,
                y_spec,
                pl.BlockSpec((1, 8, half), lambda b, jj, sc: (sc[2 + b], 0, sc[1])),
                pl.BlockSpec((1, 8, half), lambda b, jj, sc: (0, 0, col(jj, sc))),
            ],
            out_specs=block_outs(2, lambda b, jj, sc: (0, 0, 0, 0)),
        ),
        out_shape=out_shapes(2),
        name="near_blocks",
    )(scal1, up1, dn1, own, oth, stats, stats)

    low_half = (g < n_genes // 2).astype(jnp.int32)
    scal2 = jnp.stack([k, h, low_half, jnp.int32(0)]).astype(jnp.int32)
    y_spec = pl.BlockSpec((half_cells, half), lambda b, jj, sc: (sc[2], col(jj, sc)))
    w2 = pl.pallas_call(
        functools.partial(far_body, total=total),
        grid_spec=pltpu.PrefetchScalarGridSpec(
            num_scalar_prefetch=1,
            grid=(2, 2),
            in_specs=[
                x_spec,
                x_spec,
                y_spec,
                y_spec,
                x_spec,
                x_spec,
                pl.BlockSpec((1, 8, half), lambda b, jj, sc: (2, 0, sc[1])),
                pl.BlockSpec((1, 8, half), lambda b, jj, sc: (b, 0, col(jj, sc))),
            ],
            out_specs=block_outs(2, lambda b, jj, sc: (0, 0, 0, 0)),
            scratch_shapes=[pltpu.VMEM((half, half), f32), pltpu.VMEM((8, half), f32)],
        ),
        out_shape=out_shapes(2),
        name="far_blocks",
    )(scal2, up2, dn2, own, oth, near, near_other, stats, stats)

    def reduce_tiles(w):
        return [w[0]] + [send(w[j], lambda k, h, g, j=j: (k ^ j, h, g)) for j in (1, 2, 3)]

    small = shape((2, tile, tile), bf16)

    def turn(parts, turns, keeps):
        n = parts[0].shape[0]
        n_out = sum(v is not None for v in turns + keeps)
        return pl.pallas_call(
            functools.partial(turn_body, turns=turns, keeps=keeps),
            in_specs=[scalars()] + [whole()] * 4,
            out_specs=[whole()] * (1 + n_out),
            out_shape=[shape((n, 2, tile, tile), f32)] + [small] * n_out,
            name="sum_tiles",
        )(where, *parts)

    (t0,) = turn(reduce_tiles(w0), [None], [None])
    t1, e_up, e_dn = turn(reduce_tiles(w1), [0, 1], [None, None])
    t2, e_two, e_three, k_three = turn(reduce_tiles(w2), [0, 1], [None, 2])

    side = lambda f: (lambda k, h, g: (k, h ^ (k // 2), f(g)) if f(g) is not None else None)
    rd = send(e_up, side(lambda g: g - 1))
    ru = send(e_dn, side(lambda g: g + 1))
    r2 = send(e_two, side(lambda g: g ^ 2))
    inner = lambda g: 0 < g < last
    r3f = send(e_three, side(lambda g: (g ^ 2) if inner(g) else None))
    r3n = send(k_three, lambda k, h, g: (k, h, g ^ 1) if inner(g) else None)

    early = pl.pallas_call(
        early_body,
        in_specs=[scalars()] + [whole()] * 4,
        out_specs=[whole()] * 4,
        out_shape=[small] * 4,
        name="early_tiles",
    )(where, t0, t1, ru, rd)
    late = pl.pallas_call(
        late_body,
        in_specs=[scalars()] + [whole()] * 4,
        out_specs=[whole()] * 4,
        out_shape=[small] * 4,
        name="late_tiles",
    )(where, t2, r2, r3f, r3n)

    is_early = lambda q, g: -1 <= q - g <= 1
    got_early, got_late = [early[0]], [late[0]]
    for j in range(1, 4):
        got_early.append(
            send(early[j], lambda k, h, g, j=j: (k ^ j, h, g) if is_early(k ^ j, g) else None)
        )
        got_late.append(
            send(late[j], lambda k, h, g, j=j: (k ^ j, h, g) if not is_early(k ^ j, g) else None)
        )
    scal3 = jnp.stack([(2 * h) ^ k, (jnp.abs(k - g) <= 1).astype(jnp.int32)]).astype(jnp.int32)
    adjacency, row_sums = pl.pallas_call(
        place_body,
        in_specs=[scalars()] + [whole()] * 8,
        out_specs=[whole()] * 2,
        out_shape=[shape((half, width), f32), shape((half, 1), f32)],
        name="place_tiles",
    )(scal3, *got_early, *got_late)
    part = row_sums[:, 0]
    peers = [send(part, lambda k, h, g, d=d: (k, h, g ^ d)) for d in (1, 2, 3)]
    connectivity = (part + peers[0]) + (peers[1] + peers[2])
    return (adjacency, connectivity)


def folded(counts, library):
    return folded_shards(counts, library)


def solution(mesh):
    cells, genes = mesh.shape["cells"], mesh.shape["genes"]
    folds = genes == 4 and cells == 2 * genes
    return jax.shard_map(
        folded if folds else general_shards,
        mesh=mesh,
        in_specs=(P("cells", "genes"), P("cells")),
        out_specs=(P("cells", "genes"), P("cells")),
        check_vma=False,
    )
```

```python
import functools

import jax
import jax.numpy as jnp
from jax import lax
from jax.experimental import pallas as pl
from jax.experimental.pallas import tpu as pltpu
from jax.sharding import PartitionSpec as P


AXES = ("cells", "genes")


def normalize(counts, library):
    factor = 10000.0 / library.astype(jnp.float32)
    return jnp.log1p(counts.astype(jnp.float32) * factor[:, None]).astype(jnp.bfloat16)


def cross_product(left, right):
    return lax.dot_general(
        left, right, (((0,), (0,)), ((), ())), preferred_element_type=jnp.float32
    )


def general_shards(counts, library):
    own_block = normalize(counts, library)
    col_width = own_block.shape[1]
    cell_groups = lax.axis_size("cells")
    gene_total = col_width * lax.axis_size("genes")
    row_width = gene_total // cell_groups
    total_cells = float(counts.shape[0] * cell_groups)
    widened = own_block.astype(jnp.float32)
    local_sums = jnp.sum(widened, axis=0)
    local_squares = jnp.sum(widened * widened, axis=0)
    block_sums, block_squares = lax.psum((local_sums, local_squares), "cells")
    gene_sums, gene_squares = (
        lax.all_gather(block_sums, "genes", axis=0, tiled=True),
        lax.all_gather(block_squares, "genes", axis=0, tiled=True),
    )
    full_block = lax.all_gather(own_block, "genes", axis=1, tiled=True)
    gram_tile = lax.psum_scatter(
        cross_product(full_block, own_block), "cells", scatter_dimension=0, tiled=True
    )
    means = gene_sums / total_cells
    variances = gene_squares / total_cells - means * means
    scales = lax.rsqrt(variances + 1e-05)
    row_first = lax.axis_index("cells") * row_width
    col_first = lax.axis_index("genes") * col_width
    row_means = lax.dynamic_slice_in_dim(means, row_first, row_width, 0)
    col_means = lax.dynamic_slice_in_dim(means, col_first, col_width, 0)
    row_scales = lax.dynamic_slice_in_dim(scales, row_first, row_width, 0)
    col_scales = lax.dynamic_slice_in_dim(scales, col_first, col_width, 0)
    correlation = (
        (gram_tile / total_cells - row_means[:, None] * col_means[None, :])
        * row_scales[:, None]
        * col_scales[None, :]
    )
    powered = correlation**6
    row_index = row_first + jnp.arange(row_width, dtype=jnp.int32)[:, None]
    col_index = col_first + jnp.arange(col_width, dtype=jnp.int32)[None, :]
    adjacency = jnp.where(row_index == col_index, jnp.float32(0.0), powered)
    connectivity = lax.psum(jnp.sum(adjacency, axis=1), "genes")
    return (adjacency, connectivity)


def encode(x):
    return (x * jnp.abs(x) * (x * x)).astype(jnp.bfloat16)


def decode(y):
    y = y.astype(jnp.float32)
    root = lax.rsqrt(lax.rsqrt(jnp.abs(y)))
    return jnp.where(y < 0, -root, root)


def plain(left, right):
    return jnp.dot(left, right, preferred_element_type=jnp.float32)


def put_tiles(products, sums, s_ref, jj, blk, rst, cst, cells, total, own_ref, sends):
    odd = s_ref[CHIP] % 2
    row_side = rst.T
    mr, sr = row_side[:, 0:1], row_side[:, 1:2] * (1.0 / total)
    sx = sums(rst).reshape(1, -1)
    sx = jnp.broadcast_to(sx, (8, sx.shape[1])).T[:, 0:1]
    mc, sc = cst[0:1], cst[1:2]
    rest = sums(cst) - cells * mc
    t = sr.shape[0] // 2
    tiles = [[None, None], [None, None]]
    for c in range(2):
        lanes = slice(c * t, c * t + t)
        p = products(c)
        p = (p - sx * mc[:, lanes] - mr * rest[:, lanes]) * sr * sc[:, lanes]
        tiles[0][c], tiles[1][c] = p[:t], p[t:]
    for b in range(2):
        for i in range(2):
            tile = jnp.where(odd == 0, tiles[i][i ^ b], tiles[i][1 - (i ^ b)])
            coded = encode(tile)

            @pl.when(jj == 0)
            def _():
                if b == 0:
                    own_ref[blk, i] = tile
                else:
                    sends[0][blk, i] = coded

            @pl.when(jj == 1)
            def _():
                sends[1 + b][blk, i] = coded


def diagonal_body(s_ref, xa, xb, y0, y1, rst, cst, own_ref, o1, o2, o3, xs, ys, *, total):
    jj = pl.program_id(0)
    n = y0.shape[0] // 2
    t = y0.shape[1] // 2

    @pl.when(jj == 0)
    def _():
        xs[:, : 2 * n] = xa[...]
        xs[:, 2 * n :] = xb[...]

    for q in range(2):
        ys[2 * q * n : (2 * q + 1) * n] = y0[q * n : q * n + n]
        ys[(2 * q + 1) * n : (2 * q + 2) * n] = y1[q * n : q * n + n]
    put_tiles(
        lambda c: plain(xs[...], ys[:, c * t : c * t + t]),
        lambda st: st[2:3] + st[3:4],
        s_ref, jj, 0, rst[0], cst[0], 4.0 * n, total, own_ref, (o1, o2, o3),
    )


def near_body(s_ref, xa, xb, y0, y1, rst, cst, own_ref, o1, o2, o3, xs, ys, *, total):
    blk, jj = pl.program_id(0), pl.program_id(1)
    n = y0.shape[0]
    t = y0.shape[1] // 2

    @pl.when((jj == 0) & (blk == 0))
    def _():
        xs[...] = xa[...]

    @pl.when((jj == 0) & (blk == 1))
    def _():
        xs[...] = xb[...]

    ys[:n] = y0[...]
    ys[n:] = y1[...]
    put_tiles(
        lambda c: plain(xs[...], ys[:, c * t : c * t + t]),
        lambda st: jnp.where(blk == 0, st[2:3], st[3:4]),
        s_ref, jj, blk, rst[0], cst[0], 2.0 * n, total, own_ref, (o1, o2, o3),
    )


def far_body(s_ref, xa, xb, y0, y1, na, nb, rst, cst, own_ref, o1, o2, o3, xs, ys, *, total):
    blk, jj = pl.program_id(0), pl.program_id(1)
    n = y0.shape[0]
    t = y0.shape[1] // 2
    low = s_ref[LOW]

    @pl.when((jj == 0) & (blk == 0) & (low == 0))
    def _():
        xs[...] = xa[...]

    @pl.when((jj == 0) & (blk == 0) & (low == 1))
    def _():
        xs[...] = xb[...]

    other = (s_ref[CHIP] // 2) ^ jj

    @pl.when(blk == 0)
    def _():
        ys[:n] = y0[...]
        ys[n:] = y1[...]

    @pl.when((blk == 1) & (other == 0))
    def _():
        ys[...] = na[...]

    @pl.when((blk == 1) & (other == 1))
    def _():
        ys[:n] = nb[n:]
        ys[n:] = nb[:n]

    put_tiles(
        lambda c: plain(xs[...], ys[:, c * t : c * t + t]),
        lambda st: jnp.where(low == 0, st[2:3], st[3:4]),
        s_ref, jj, blk, rst[0], cst[0], 2.0 * n, total, own_ref, (o1, o2, o3),
    )


CHIP, CORE, PLANE, PLANES, LOW, LOWER, _, SHIFT, EARLY = range(9)


def turn_body(s_ref, own, r1, r2, r3, *outs, turns, keeps):
    odd = s_ref[CHIP] % 2
    t_ref, rest = outs[0], outs[1:]
    for n in range(own.shape[0]):
        for i in range(2):
            v = own[n, i] + decode(r1[n, i]) + decode(r2[n, i]) + decode(r3[n, i])
            t_ref[n, i] = v
            if keeps[n] is not None:
                rest[keeps[n]][i] = encode(v)
            if turns[n] is not None:
                w = encode(v.T)
                dst = rest[turns[n]]

                @pl.when(odd == 0)
                def _():
                    dst[i] = w

                @pl.when(odd == 1)
                def _():
                    dst[1 - i] = w


def power(v):
    v2 = v * v
    return v2 * v2 * v2


def put_slot(outs, where, i, value):
    for j, o in enumerate(outs):

        @pl.when(where == j)
        def _():
            o[i] = value


def early_body(s_ref, t0, t1, ru, rd, *outs):
    k, g = s_ref[CHIP], s_ref[PLANE]
    n = t0.shape[-1]
    for i in range(2):
        own = power(t0[0, i])
        same = lax.broadcasted_iota(jnp.int32, (n, n), 0) == lax.broadcasted_iota(
            jnp.int32, (n, n), 1
        )
        own = jnp.where(same & (k == 0), 0.0, own).astype(jnp.bfloat16)
        put_slot(outs, g ^ k, i, own)
        low = power(t1[0, i] + decode(ru[i])).astype(jnp.bfloat16)
        put_slot(outs, jnp.where(g > 0, (g - 1) ^ k, -1), i, low)
        high = power(t1[1, i] + decode(rd[i])).astype(jnp.bfloat16)
        put_slot(outs, jnp.where(g < s_ref[PLANES] - 1, (g + 1) ^ k, -1), i, high)


def late_body(s_ref, t2, r2, rf, rn, *outs):
    k, g = s_ref[CHIP], s_ref[PLANE]
    outer = (g == 0) | (g == s_ref[PLANES] - 1)
    for i in range(2):
        two = power(t2[0, i] + decode(r2[i])).astype(jnp.bfloat16)
        put_slot(outs, g ^ 2 ^ k, i, two)
        three = power(decode(rf[i]) + decode(rn[i])).astype(jnp.bfloat16)
        put_slot(outs, jnp.where(outer, g ^ 3 ^ k, -1), i, three)


def place_body(s_ref, e0, e1, e2, e3, l0, l1, l2, l3, out_ref, sum_ref):
    x = s_ref[SHIFT]
    is_early = s_ref[EARLY]
    early, late = (e0, e1, e2, e3), (l0, l1, l2, l3)
    t = e0.shape[-1]

    def place(tiles):
        for i in range(2):
            total = jnp.zeros((t, 1), jnp.float32)
            for c in range(4):
                v = tiles[c ^ i][i]
                for m in range(1, 4):
                    v = jnp.where(x == m, tiles[c ^ i ^ m][i], v)
                v = v.astype(jnp.float32)
                out_ref[i * t : i * t + t, c * t : c * t + t] = v
                total = total + jnp.sum(v, axis=1, keepdims=True)
            sum_ref[i * t : i * t + t, :] = total

    @pl.when(is_early == 1)
    def _():
        place(early)

    @pl.when(is_early == 0)
    def _():
        place(late)


def pay_body(s_ref, a, *refs):
    out_a, out_b = refs[-2:]
    n = a.shape[0] // 2
    out_a[...] = a[:n].T
    out_b[...] = a[n:].T


def limit(mib):
    return pltpu.CompilerParams(vmem_limit_bytes=mib * 1024 * 1024)


def whole():
    return pl.BlockSpec(memory_space=pltpu.VMEM)


def scalars():
    return pl.BlockSpec(memory_space=pltpu.SMEM)


def folded_shards(counts, library):
    rows, width = counts.shape
    n_cells = lax.axis_size("cells")
    n_genes = lax.axis_size("genes")
    cores = n_cells // n_genes
    total = float(rows * n_cells)
    half_cells = rows // 2
    half = width // cores
    tile = half // 2
    g = lax.axis_index("genes")
    c = lax.axis_index("cells")
    k, h = c // cores, c % cores

    def perm(f):
        pairs = []
        for ci in range(n_cells):
            for gi in range(n_genes):
                d = f(ci // cores, ci % cores, gi)
                if d is not None and 0 <= d[2] < n_genes:
                    pairs.append((ci * n_genes + gi, (d[0] * cores + d[1]) * n_genes + d[2]))
        return pairs

    def send(x, f):
        return lax.ppermute(x, AXES, perm(f))

    flip = lambda k, h, g: (k, h ^ 1, g)
    bf16, f32 = jnp.bfloat16, jnp.float32
    shape = jax.ShapeDtypeStruct

    last = n_genes - 1
    own = normalize(counts, library)
    oth = send(own, flip)
    info = jnp.stack(
        [
            k,
            h,
            g,
            jnp.int32(n_genes),
            (g < n_genes // 2).astype(jnp.int32),
            jnp.where(g > 0, g ^ (g - 1), 0),
            jnp.where(g < last, g ^ (g + 1), 0),
            (2 * h) ^ k,
            (jnp.abs(k - g) <= 1).astype(jnp.int32),
        ]
    ).astype(jnp.int32)

    pay_in = pl.BlockSpec((rows, half), lambda i, sc: (0, sc[CORE]))
    pay_shapes = [shape((half, rows), bf16)] * 2

    def turn_payload(block, part, before):
        return pl.pallas_call(
            pay_body,
            grid_spec=pltpu.PrefetchScalarGridSpec(
                num_scalar_prefetch=1,
                grid=(1,),
                in_specs=[pay_in] + [pl.BlockSpec(memory_space=pl.ANY)] * len(before),
                out_specs=[pl.BlockSpec((half, half_cells), lambda i, sc: (0, part))] * 2,
            ),
            out_shape=pay_shapes,
            input_output_aliases={2 + n: n for n in range(len(before))},
            compiler_params=limit(8),
            name="turn_payload",
        )(info, block, *before)

    pay_a, pay_b = turn_payload(oth, 1, turn_payload(own, 0, []))
    up1 = send(pay_a, lambda k, h, g: (k, h, g + 1))
    dn1 = send(pay_b, lambda k, h, g: (k, h, g - 1))
    widened = own.astype(f32)
    halves = jnp.sum(widened.reshape(2, half_cells, width), axis=1)
    squares = jnp.sum(widened * widened, axis=0)
    chip_halves = halves + send(halves, flip)
    sums = lax.psum(jnp.stack([halves[0] + halves[1], squares]), "cells")
    means = sums[0] / total
    variances = sums[1] / total - means * means
    mine = jnp.concatenate(
        [means[None], lax.rsqrt(variances + 1e-05)[None], chip_halves, jnp.zeros((4, width), f32)]
    )
    afar = [send(mine, lambda k, h, g, d=d: (k, h, g ^ d)) for d in (1, 2, 3)]
    own_stats = mine[None]
    stats = jnp.stack([mine] + afar)
    corner = (jnp.where(g == 0, half_cells, 0), h * half)
    end = jnp.concatenate([lax.dynamic_slice(a, corner, (half_cells, half)) for a in (own, oth)])
    near = send(
        end, lambda k, h, g: (k, h, 1) if g == 0 else ((k, h, g - 1) if g == last else None)
    )

    def block_outs(n):
        spec = pl.BlockSpec((n, 2, tile, tile), lambda *_: (0, 0, 0, 0))
        return [spec] * 4

    def out_shapes(n):
        return [shape((n, 2, tile, tile), f32)] + [shape((n, 2, tile, tile), bf16)] * 3

    def stat_spec(m):
        return pl.BlockSpec((1, 8, half), m)

    col = lambda jj, sc: sc[CORE] ^ (sc[CHIP] // 2) ^ jj
    x_spec = pl.BlockSpec((half, rows), lambda jj, sc: (0, 0))
    y_spec = pl.BlockSpec((rows, half), lambda jj, sc: (0, col(jj, sc)))
    w0 = pl.pallas_call(
        functools.partial(diagonal_body, total=total),
        grid_spec=pltpu.PrefetchScalarGridSpec(
            num_scalar_prefetch=1,
            grid=(2,),
            in_specs=[
                x_spec,
                x_spec,
                y_spec,
                y_spec,
                stat_spec(lambda jj, sc: (0, 0, sc[CORE])),
                stat_spec(lambda jj, sc: (0, 0, col(jj, sc))),
            ],
            out_specs=block_outs(1),
            scratch_shapes=[pltpu.VMEM((half, 2 * rows), bf16), pltpu.VMEM((2 * rows, half), bf16)],
        ),
        out_shape=out_shapes(1),
        compiler_params=limit(24),
        name="diagonal_block",
    )(info, pay_a, pay_b, own, oth, own_stats, own_stats)

    up2 = send(up1, lambda k, h, g: (k, h, g + 1) if g > 0 else None)
    dn2 = send(dn1, lambda k, h, g: (k, h, g - 1) if g < last else None)
    near_other = send(near, flip)

    x_spec = pl.BlockSpec((half, rows), lambda b, jj, sc: (0, 0))
    scratch = [pltpu.VMEM((half, rows), bf16), pltpu.VMEM((rows, half), bf16)]
    y_spec = pl.BlockSpec((half_cells, half), lambda b, jj, sc: (b, col(jj, sc)))
    w1 = pl.pallas_call(
        functools.partial(near_body, total=total),
        grid_spec=pltpu.PrefetchScalarGridSpec(
            num_scalar_prefetch=1,
            grid=(2, 2),
            in_specs=[
                x_spec,
                x_spec,
                y_spec,
                y_spec,
                stat_spec(lambda b, jj, sc: (sc[LOWER + b], 0, sc[CORE])),
                stat_spec(lambda b, jj, sc: (0, 0, col(jj, sc))),
            ],
            out_specs=block_outs(2),
            scratch_shapes=scratch,
        ),
        out_shape=out_shapes(2),
        compiler_params=limit(20),
        name="near_blocks",
    )(info, up1, dn1, own, oth, stats, stats)

    n_spec = pl.BlockSpec((rows, half), lambda b, jj, sc: (0, 0))
    y_spec = pl.BlockSpec((half_cells, half), lambda b, jj, sc: (sc[LOW], col(jj, sc)))
    w2 = pl.pallas_call(
        functools.partial(far_body, total=total),
        grid_spec=pltpu.PrefetchScalarGridSpec(
            num_scalar_prefetch=1,
            grid=(2, 2),
            in_specs=[
                x_spec,
                x_spec,
                y_spec,
                y_spec,
                n_spec,
                n_spec,
                stat_spec(lambda b, jj, sc: (2, 0, sc[CORE])),
                stat_spec(lambda b, jj, sc: (b, 0, col(jj, sc))),
            ],
            out_specs=block_outs(2),
            scratch_shapes=scratch,
        ),
        out_shape=out_shapes(2),
        compiler_params=limit(20),
        name="far_blocks",
    )(info, up2, dn2, own, oth, near, near_other, stats, stats)

    def reduce_tiles(w):
        return [w[0]] + [send(w[j], lambda k, h, g, j=j: (k ^ j, h, g)) for j in (1, 2, 3)]

    small = shape((2, tile, tile), bf16)

    def turn(parts, turns, keeps):
        n = parts[0].shape[0]
        n_out = sum(v is not None for v in turns + keeps)
        return pl.pallas_call(
            functools.partial(turn_body, turns=turns, keeps=keeps),
            in_specs=[scalars()] + [whole()] * 4,
            out_specs=[whole()] * (1 + n_out),
            out_shape=[shape((n, 2, tile, tile), f32)] + [small] * n_out,
            compiler_params=limit(12),
            name="sum_tiles",
        )(info, *parts)

    (t0,) = turn(reduce_tiles(w0), [None], [None])
    t1, e_up, e_dn = turn(reduce_tiles(w1), [0, 1], [None, None])
    t2, e_two, e_three, k_three = turn(reduce_tiles(w2), [0, 1], [None, 2])

    side = lambda f: (lambda k, h, g: (k, h ^ (k // 2), f(g)) if f(g) is not None else None)
    rd = send(e_up, side(lambda g: g - 1))
    ru = send(e_dn, side(lambda g: g + 1))
    r2 = send(e_two, side(lambda g: g ^ 2))
    inner = lambda g: 0 < g < last
    r3f = send(e_three, side(lambda g: (g ^ 2) if inner(g) else None))
    r3n = send(k_three, lambda k, h, g: (k, h, g ^ 1) if inner(g) else None)

    early = pl.pallas_call(
        early_body,
        in_specs=[scalars()] + [whole()] * 4,
        out_specs=[whole()] * 4,
        out_shape=[small] * 4,
        compiler_params=limit(10),
        name="early_tiles",
    )(info, t0, t1, ru, rd)
    late = pl.pallas_call(
        late_body,
        in_specs=[scalars()] + [whole()] * 4,
        out_specs=[whole()] * 4,
        out_shape=[small] * 4,
        compiler_params=limit(10),
        name="late_tiles",
    )(info, t2, r2, r3f, r3n)

    is_early = lambda q, g: -1 <= q - g <= 1
    got_early, got_late = [early[0]], [late[0]]
    for j in range(1, 4):
        got_early.append(
            send(early[j], lambda k, h, g, j=j: (k ^ j, h, g) if is_early(k ^ j, g) else None)
        )
        got_late.append(
            send(late[j], lambda k, h, g, j=j: (k ^ j, h, g) if not is_early(k ^ j, g) else None)
        )
    adjacency, row_sums = pl.pallas_call(
        place_body,
        in_specs=[scalars()] + [whole()] * 8,
        out_specs=[whole()] * 2,
        out_shape=[shape((half, width), f32), shape((half, 1), f32)],
        compiler_params=limit(12),
        name="place_tiles",
    )(info, *got_early, *got_late)
    part = row_sums[:, 0]
    peers = [send(part, lambda k, h, g, d=d: (k, h, g ^ d)) for d in (1, 2, 3)]
    connectivity = (part + peers[0]) + (peers[1] + peers[2])
    return (adjacency, connectivity)


def folded(counts, library):
    return folded_shards(counts, library)


def solution(mesh):
    cells, genes = mesh.shape["cells"], mesh.shape["genes"]
    folds = genes == 4 and cells == 2 * genes
    return jax.shard_map(
        folded if folds else general_shards,
        mesh=mesh,
        in_specs=(P("cells", "genes"), P("cells")),
        out_specs=(P("cells", "genes"), P("cells")),
        check_vma=False,
    )
```

```python
import functools

import jax
import jax.numpy as jnp
from jax import lax
from jax.experimental import pallas as pl
from jax.experimental.pallas import tpu as pltpu
from jax.sharding import PartitionSpec as P


AXES = ("cells", "genes")


def normalize(counts, library):
    factor = 10000.0 / library.astype(jnp.float32)
    return jnp.log1p(counts.astype(jnp.float32) * factor[:, None]).astype(jnp.bfloat16)


def cross_product(left, right):
    return lax.dot_general(
        left, right, (((0,), (0,)), ((), ())), preferred_element_type=jnp.float32
    )


def general_shards(counts, library):
    own_block = normalize(counts, library)
    col_width = own_block.shape[1]
    cell_groups = lax.axis_size("cells")
    gene_total = col_width * lax.axis_size("genes")
    row_width = gene_total // cell_groups
    total_cells = float(counts.shape[0] * cell_groups)
    widened = own_block.astype(jnp.float32)
    local_sums = jnp.sum(widened, axis=0)
    local_squares = jnp.sum(widened * widened, axis=0)
    block_sums, block_squares = lax.psum((local_sums, local_squares), "cells")
    gene_sums, gene_squares = (
        lax.all_gather(block_sums, "genes", axis=0, tiled=True),
        lax.all_gather(block_squares, "genes", axis=0, tiled=True),
    )
    full_block = lax.all_gather(own_block, "genes", axis=1, tiled=True)
    gram_tile = lax.psum_scatter(
        cross_product(full_block, own_block), "cells", scatter_dimension=0, tiled=True
    )
    means = gene_sums / total_cells
    variances = gene_squares / total_cells - means * means
    scales = lax.rsqrt(variances + 1e-05)
    row_first = lax.axis_index("cells") * row_width
    col_first = lax.axis_index("genes") * col_width
    row_means = lax.dynamic_slice_in_dim(means, row_first, row_width, 0)
    col_means = lax.dynamic_slice_in_dim(means, col_first, col_width, 0)
    row_scales = lax.dynamic_slice_in_dim(scales, row_first, row_width, 0)
    col_scales = lax.dynamic_slice_in_dim(scales, col_first, col_width, 0)
    correlation = (
        (gram_tile / total_cells - row_means[:, None] * col_means[None, :])
        * row_scales[:, None]
        * col_scales[None, :]
    )
    powered = correlation**6
    row_index = row_first + jnp.arange(row_width, dtype=jnp.int32)[:, None]
    col_index = col_first + jnp.arange(col_width, dtype=jnp.int32)[None, :]
    adjacency = jnp.where(row_index == col_index, jnp.float32(0.0), powered)
    connectivity = lax.psum(jnp.sum(adjacency, axis=1), "genes")
    return (adjacency, connectivity)


def encode(x):
    return (x * jnp.abs(x) * (x * x)).astype(jnp.bfloat16)


def decode(y):
    y = y.astype(jnp.float32)
    root = lax.rsqrt(lax.rsqrt(jnp.abs(y)))
    return jnp.where(y < 0, -root, root)


def plain(left, right):
    return jnp.dot(left, right, preferred_element_type=jnp.float32)


def put_tiles(products, sums, s_ref, jj, blk, rst, cst, cells, total, own_ref, sends):
    odd = s_ref[CHIP] % 2
    row_side = rst.T
    mr, sr = row_side[:, 0:1], row_side[:, 1:2] * (1.0 / total)
    sx = sums(rst).reshape(1, -1)
    sx = jnp.broadcast_to(sx, (8, sx.shape[1])).T[:, 0:1]
    mc, sc = cst[0:1], cst[1:2]
    rest = sums(cst) - cells * mc
    t = sr.shape[0] // 2
    tiles = [[None, None], [None, None]]
    for c in range(2):
        lanes = slice(c * t, c * t + t)
        p = products(c)
        p = (p - sx * mc[:, lanes] - mr * rest[:, lanes]) * sr * sc[:, lanes]
        tiles[0][c], tiles[1][c] = p[:t], p[t:]
    for b in range(2):
        for i in range(2):
            tile = jnp.where(odd == 0, tiles[i][i ^ b], tiles[i][1 - (i ^ b)])
            coded = encode(tile)

            @pl.when(jj == 0)
            def _():
                if b == 0:
                    own_ref[blk, i] = tile
                else:
                    sends[0][blk, i] = coded

            @pl.when(jj == 1)
            def _():
                sends[1 + b][blk, i] = coded


def diagonal_body(s_ref, xa, xb, y0, y1, rst, cst, own_ref, o1, o2, o3, xs, ys, *, total):
    jj = pl.program_id(0)
    n = y0.shape[0] // 2
    t = y0.shape[1] // 2

    @pl.when(jj == 0)
    def _():
        xs[:, : 2 * n] = xa[...]
        xs[:, 2 * n :] = xb[...]

    for q in range(2):
        ys[2 * q * n : (2 * q + 1) * n] = y0[q * n : q * n + n]
        ys[(2 * q + 1) * n : (2 * q + 2) * n] = y1[q * n : q * n + n]
    put_tiles(
        lambda c: plain(xs[...], ys[:, c * t : c * t + t]),
        lambda st: st[2:3] + st[3:4],
        s_ref, jj, 0, rst[0], cst[0], 4.0 * n, total, own_ref, (o1, o2, o3),
    )


def near_body(s_ref, xa, xb, y0, y1, rst, cst, own_ref, o1, o2, o3, xs, ys, *, total):
    blk, jj = pl.program_id(0), pl.program_id(1)
    n = y0.shape[0]
    t = y0.shape[1] // 2

    @pl.when((jj == 0) & (blk == 0))
    def _():
        xs[...] = xa[...]

    @pl.when((jj == 0) & (blk == 1))
    def _():
        xs[...] = xb[...]

    ys[:n] = y0[...]
    ys[n:] = y1[...]
    put_tiles(
        lambda c: plain(xs[...], ys[:, c * t : c * t + t]),
        lambda st: jnp.where(blk == 0, st[2:3], st[3:4]),
        s_ref, jj, blk, rst[0], cst[0], 2.0 * n, total, own_ref, (o1, o2, o3),
    )


def pick_far(s_ref, xa, xb, xs):
    @pl.when((pl.program_id(0) == 0) & (s_ref[LOW] == 0))
    def _():
        xs[...] = xa[...]

    @pl.when((pl.program_id(0) == 0) & (s_ref[LOW] == 1))
    def _():
        xs[...] = xb[...]


def put_far(s_ref, rst, cst, outs, xs, ys, total):
    t = ys.shape[1] // 2
    put_tiles(
        lambda c: plain(xs[...], ys[:, c * t : c * t + t]),
        lambda st: jnp.where(s_ref[LOW] == 0, st[2:3], st[3:4]),
        s_ref, pl.program_id(0), 0, rst[0], cst[0], float(xs.shape[1]), total, outs[0], outs[1:],
    )


def far_body(s_ref, xa, xb, y0, y1, rst, cst, own_ref, o1, o2, o3, xs, ys, *, total):
    n = y0.shape[0]
    pick_far(s_ref, xa, xb, xs)
    ys[:n] = y0[...]
    ys[n:] = y1[...]
    put_far(s_ref, rst, cst, (own_ref, o1, o2, o3), xs, ys, total)


def ends_body(s_ref, xa, xb, na, nb, rst, cst, own_ref, o1, o2, o3, xs, ys, *, total):
    n = na.shape[0] // 2
    pick_far(s_ref, xa, xb, xs)
    other = (s_ref[CHIP] // 2) ^ pl.program_id(0)

    @pl.when(other == 0)
    def _():
        ys[...] = na[...]

    @pl.when(other == 1)
    def _():
        ys[:n] = nb[n:]
        ys[n:] = nb[:n]

    put_far(s_ref, rst, cst, (own_ref, o1, o2, o3), xs, ys, total)


CHIP, CORE, PLANE, PLANES, LOW, LOWER, _, SHIFT, EARLY = range(9)


def turn_body(s_ref, own, r1, r2, r3, *outs, turns, keeps):
    odd = s_ref[CHIP] % 2
    t_ref, rest = outs[0], outs[1:]
    for n in range(own.shape[0]):
        for i in range(2):
            v = own[n, i] + decode(r1[n, i]) + decode(r2[n, i]) + decode(r3[n, i])
            t_ref[n, i] = v
            if keeps[n] is not None:
                rest[keeps[n]][i] = encode(v)
            if turns[n] is not None:
                w = encode(v.T)
                dst = rest[turns[n]]

                @pl.when(odd == 0)
                def _():
                    dst[i] = w

                @pl.when(odd == 1)
                def _():
                    dst[1 - i] = w


def power(v):
    v2 = v * v
    return v2 * v2 * v2


def put_slot(outs, where, i, value):
    for j, o in enumerate(outs):

        @pl.when(where == j)
        def _():
            o[i] = value


def early_body(s_ref, t0, t1, ru, rd, *outs):
    k, g = s_ref[CHIP], s_ref[PLANE]
    n = t0.shape[-1]
    for i in range(2):
        own = power(t0[0, i])
        same = lax.broadcasted_iota(jnp.int32, (n, n), 0) == lax.broadcasted_iota(
            jnp.int32, (n, n), 1
        )
        own = jnp.where(same & (k == 0), 0.0, own).astype(jnp.bfloat16)
        put_slot(outs, g ^ k, i, own)
        low = power(t1[0, i] + decode(ru[i])).astype(jnp.bfloat16)
        put_slot(outs, jnp.where(g > 0, (g - 1) ^ k, -1), i, low)
        high = power(t1[1, i] + decode(rd[i])).astype(jnp.bfloat16)
        put_slot(outs, jnp.where(g < s_ref[PLANES] - 1, (g + 1) ^ k, -1), i, high)


def late_body(s_ref, t2, r2, rf, rn, *outs):
    k, g = s_ref[CHIP], s_ref[PLANE]
    outer = (g == 0) | (g == s_ref[PLANES] - 1)
    for i in range(2):
        two = power(t2[0, i] + decode(r2[i])).astype(jnp.bfloat16)
        put_slot(outs, g ^ 2 ^ k, i, two)
        three = power(decode(rf[i]) + decode(rn[i])).astype(jnp.bfloat16)
        put_slot(outs, jnp.where(outer, g ^ 3 ^ k, -1), i, three)


def place_body(s_ref, e0, e1, e2, e3, l0, l1, l2, l3, out_ref, sum_ref):
    x = s_ref[SHIFT]
    is_early = s_ref[EARLY]
    early, late = (e0, e1, e2, e3), (l0, l1, l2, l3)
    t = e0.shape[-1]

    def place(tiles):
        for i in range(2):
            total = jnp.zeros((t, 1), jnp.float32)
            for c in range(4):
                v = tiles[c ^ i][i]
                for m in range(1, 4):
                    v = jnp.where(x == m, tiles[c ^ i ^ m][i], v)
                v = v.astype(jnp.float32)
                out_ref[i * t : i * t + t, c * t : c * t + t] = v
                total = total + jnp.sum(v, axis=1, keepdims=True)
            sum_ref[i * t : i * t + t, :] = total

    @pl.when(is_early == 1)
    def _():
        place(early)

    @pl.when(is_early == 0)
    def _():
        place(late)


def pay_body(s_ref, a, *refs):
    out_a, out_b, out_n = refs[-3:]
    n = a.shape[0] // 2
    out_a[...] = a[:n].T
    out_b[...] = a[n:].T
    first = pl.multiple_of(jnp.where(s_ref[PLANE] == 0, n, 0), n)
    out_n[...] = a[pl.ds(first, n)]


def limit(mib):
    return pltpu.CompilerParams(vmem_limit_bytes=mib * 1024 * 1024)


def whole():
    return pl.BlockSpec(memory_space=pltpu.VMEM)


def scalars():
    return pl.BlockSpec(memory_space=pltpu.SMEM)


def folded_shards(counts, library):
    rows, width = counts.shape
    n_cells = lax.axis_size("cells")
    n_genes = lax.axis_size("genes")
    cores = n_cells // n_genes
    total = float(rows * n_cells)
    half_cells = rows // 2
    half = width // cores
    tile = half // 2
    g = lax.axis_index("genes")
    c = lax.axis_index("cells")
    k, h = c // cores, c % cores

    def perm(f):
        pairs = []
        for ci in range(n_cells):
            for gi in range(n_genes):
                d = f(ci // cores, ci % cores, gi)
                if d is not None and 0 <= d[2] < n_genes:
                    pairs.append((ci * n_genes + gi, (d[0] * cores + d[1]) * n_genes + d[2]))
        return pairs

    def send(x, f):
        return lax.ppermute(x, AXES, perm(f))

    flip = lambda k, h, g: (k, h ^ 1, g)
    bf16, f32 = jnp.bfloat16, jnp.float32
    shape = jax.ShapeDtypeStruct

    last = n_genes - 1
    own = normalize(counts, library)
    oth = send(own, flip)
    info = jnp.stack(
        [
            k,
            h,
            g,
            jnp.int32(n_genes),
            (g < n_genes // 2).astype(jnp.int32),
            jnp.where(g > 0, g ^ (g - 1), 0),
            jnp.where(g < last, g ^ (g + 1), 0),
            (2 * h) ^ k,
            (jnp.abs(k - g) <= 1).astype(jnp.int32),
        ]
    ).astype(jnp.int32)

    pay_in = pl.BlockSpec((rows, half), lambda i, sc: (0, sc[CORE]))
    pay_shapes = [shape((half, rows), bf16)] * 2 + [shape((rows, half), bf16)]

    def turn_payload(block, part, before):
        return pl.pallas_call(
            pay_body,
            grid_spec=pltpu.PrefetchScalarGridSpec(
                num_scalar_prefetch=1,
                grid=(1,),
                in_specs=[pay_in] + [pl.BlockSpec(memory_space=pl.ANY)] * len(before),
                out_specs=[pl.BlockSpec((half, half_cells), lambda i, sc: (0, part))] * 2
                + [pl.BlockSpec((half_cells, half), lambda i, sc: (part, 0))],
            ),
            out_shape=pay_shapes,
            input_output_aliases={2 + n: n for n in range(len(before))},
            compiler_params=limit(8),
            name="turn_payload",
        )(info, block, *before)

    pay_a, pay_b, end = turn_payload(oth, 1, turn_payload(own, 0, []))
    up1 = send(pay_a, lambda k, h, g: (k, h, g + 1))
    dn1 = send(pay_b, lambda k, h, g: (k, h, g - 1))
    widened = own.astype(f32)
    halves = jnp.sum(widened.reshape(2, half_cells, width), axis=1)
    squares = jnp.sum(widened * widened, axis=0)
    local = jnp.concatenate([halves, squares[None]])
    chip = local + send(local, flip)
    chip_halves = chip[:2]
    pair = jnp.stack([chip[0] + chip[1], chip[2]])
    around = [send(pair, lambda k, h, g, j=j: (k ^ j, h, g)) for j in (1, 2, 3)]
    sums = (pair + around[0]) + (around[1] + around[2])
    means = sums[0] / total
    variances = sums[1] / total - means * means
    mine = jnp.concatenate(
        [means[None], lax.rsqrt(variances + 1e-05)[None], chip_halves, jnp.zeros((4, width), f32)]
    )
    afar = [send(mine, lambda k, h, g, d=d: (k, h, g ^ d)) for d in (1, 2, 3)]
    own_stats = mine[None]
    stats = jnp.stack([mine] + afar)
    near = send(
        end, lambda k, h, g: (k, h, 1) if g == 0 else ((k, h, g - 1) if g == last else None)
    )

    def block_outs(n):
        spec = pl.BlockSpec((n, 2, tile, tile), lambda *_: (0, 0, 0, 0))
        return [spec] * 4

    def out_shapes(n):
        return [shape((n, 2, tile, tile), f32)] + [shape((n, 2, tile, tile), bf16)] * 3

    def stat_spec(m):
        return pl.BlockSpec((1, 8, half), m)

    col = lambda jj, sc: sc[CORE] ^ (sc[CHIP] // 2) ^ jj
    x_spec = pl.BlockSpec((half, rows), lambda jj, sc: (0, 0))
    y_spec = pl.BlockSpec((rows, half), lambda jj, sc: (0, col(jj, sc)))
    w0 = pl.pallas_call(
        functools.partial(diagonal_body, total=total),
        grid_spec=pltpu.PrefetchScalarGridSpec(
            num_scalar_prefetch=1,
            grid=(2,),
            in_specs=[
                x_spec,
                x_spec,
                y_spec,
                y_spec,
                stat_spec(lambda jj, sc: (0, 0, sc[CORE])),
                stat_spec(lambda jj, sc: (0, 0, col(jj, sc))),
            ],
            out_specs=block_outs(1),
            scratch_shapes=[pltpu.VMEM((half, 2 * rows), bf16), pltpu.VMEM((2 * rows, half), bf16)],
        ),
        out_shape=out_shapes(1),
        compiler_params=limit(24),
        name="diagonal_block",
    )(info, pay_a, pay_b, own, oth, own_stats, own_stats)

    up2 = send(up1, lambda k, h, g: (k, h, g + 1) if g > 0 else None)
    dn2 = send(dn1, lambda k, h, g: (k, h, g - 1) if g < last else None)
    near_other = send(near, flip)

    x_spec = pl.BlockSpec((half, rows), lambda b, jj, sc: (0, 0))
    scratch = [pltpu.VMEM((half, rows), bf16), pltpu.VMEM((rows, half), bf16)]
    y_spec = pl.BlockSpec((half_cells, half), lambda b, jj, sc: (b, col(jj, sc)))
    w1 = pl.pallas_call(
        functools.partial(near_body, total=total),
        grid_spec=pltpu.PrefetchScalarGridSpec(
            num_scalar_prefetch=1,
            grid=(2, 2),
            in_specs=[
                x_spec,
                x_spec,
                y_spec,
                y_spec,
                stat_spec(lambda b, jj, sc: (sc[LOWER + b], 0, sc[CORE])),
                stat_spec(lambda b, jj, sc: (0, 0, col(jj, sc))),
            ],
            out_specs=block_outs(2),
            scratch_shapes=scratch,
        ),
        out_shape=out_shapes(2),
        compiler_params=limit(20),
        name="near_blocks",
    )(info, up1, dn1, own, oth, stats, stats)

    x_spec = pl.BlockSpec((half, rows), lambda jj, sc: (0, 0))
    n_spec = pl.BlockSpec((rows, half), lambda jj, sc: (0, 0))

    def far_call(body, others, specs, plane):
        return pl.pallas_call(
            functools.partial(body, total=total),
            grid_spec=pltpu.PrefetchScalarGridSpec(
                num_scalar_prefetch=1,
                grid=(2,),
                in_specs=[x_spec, x_spec]
                + specs
                + [
                    stat_spec(lambda jj, sc: (2, 0, sc[CORE])),
                    stat_spec(lambda jj, sc: (plane, 0, col(jj, sc))),
                ],
                out_specs=block_outs(1),
                scratch_shapes=scratch,
            ),
            out_shape=out_shapes(1),
            compiler_params=limit(20),
            name="far_block",
        )(info, up2, dn2, *others, stats, stats)

    y_spec = pl.BlockSpec((half_cells, half), lambda jj, sc: (sc[LOW], col(jj, sc)))
    w2 = far_call(far_body, [own, oth], [y_spec] * 2, 0)
    w3 = far_call(ends_body, [near, near_other], [n_spec] * 2, 1)

    def reduce_tiles(w):
        return [w[0]] + [send(w[j], lambda k, h, g, j=j: (k ^ j, h, g)) for j in (1, 2, 3)]

    small = shape((2, tile, tile), bf16)

    def turn(parts, turns, keeps):
        n = parts[0].shape[0]
        n_out = sum(v is not None for v in turns + keeps)
        return pl.pallas_call(
            functools.partial(turn_body, turns=turns, keeps=keeps),
            in_specs=[scalars()] + [whole()] * 4,
            out_specs=[whole()] * (1 + n_out),
            out_shape=[shape((n, 2, tile, tile), f32)] + [small] * n_out,
            compiler_params=limit(12),
            name="sum_tiles",
        )(info, *parts)

    (t0,) = turn(reduce_tiles(w0), [None], [None])
    t1, e_up, e_dn = turn(reduce_tiles(w1), [0, 1], [None, None])
    t2, e_two = turn(reduce_tiles(w2), [0], [None])
    _, e_three, k_three = turn(reduce_tiles(w3), [0], [1])

    side = lambda f: (lambda k, h, g: (k, h ^ (k // 2), f(g)) if f(g) is not None else None)
    rd = send(e_up, side(lambda g: g - 1))
    ru = send(e_dn, side(lambda g: g + 1))
    r2 = send(e_two, side(lambda g: g ^ 2))
    inner = lambda g: 0 < g < last
    r3f = send(e_three, side(lambda g: (g ^ 2) if inner(g) else None))
    r3n = send(k_three, lambda k, h, g: (k, h, g ^ 1) if inner(g) else None)

    early = pl.pallas_call(
        early_body,
        in_specs=[scalars()] + [whole()] * 4,
        out_specs=[whole()] * 4,
        out_shape=[small] * 4,
        compiler_params=limit(10),
        name="early_tiles",
    )(info, t0, t1, ru, rd)
    late = pl.pallas_call(
        late_body,
        in_specs=[scalars()] + [whole()] * 4,
        out_specs=[whole()] * 4,
        out_shape=[small] * 4,
        compiler_params=limit(10),
        name="late_tiles",
    )(info, t2, r2, r3f, r3n)

    is_early = lambda q, g: -1 <= q - g <= 1
    got_early, got_late = [early[0]], [late[0]]
    for j in range(1, 4):
        got_early.append(
            send(early[j], lambda k, h, g, j=j: (k ^ j, h, g) if is_early(k ^ j, g) else None)
        )
        got_late.append(
            send(late[j], lambda k, h, g, j=j: (k ^ j, h, g) if not is_early(k ^ j, g) else None)
        )
    adjacency, row_sums = pl.pallas_call(
        place_body,
        in_specs=[scalars()] + [whole()] * 8,
        out_specs=[whole()] * 2,
        out_shape=[shape((half, width), f32), shape((half, 1), f32)],
        compiler_params=limit(12),
        name="place_tiles",
    )(info, *got_early, *got_late)
    part = row_sums[:, 0]
    peers = [send(part, lambda k, h, g, d=d: (k, h, g ^ d)) for d in (1, 2, 3)]
    connectivity = (part + peers[0]) + (peers[1] + peers[2])
    return (adjacency, connectivity)


def folded(counts, library):
    return folded_shards(counts, library)


def solution(mesh):
    cells, genes = mesh.shape["cells"], mesh.shape["genes"]
    folds = genes == 4 and cells == 2 * genes
    return jax.shard_map(
        folded if folds else general_shards,
        mesh=mesh,
        in_specs=(P("cells", "genes"), P("cells")),
        out_specs=(P("cells", "genes"), P("cells")),
        check_vma=False,
    )
```

```python
import functools

import jax
import jax.numpy as jnp
from jax import lax
from jax.experimental import pallas as pl
from jax.experimental.pallas import tpu as pltpu
from jax.sharding import PartitionSpec as P


AXES = ("cells", "genes")


def normalize(counts, library):
    factor = 10000.0 / library.astype(jnp.float32)
    return jnp.log1p(counts.astype(jnp.float32) * factor[:, None]).astype(jnp.bfloat16)


def cross_product(left, right):
    return lax.dot_general(
        left, right, (((0,), (0,)), ((), ())), preferred_element_type=jnp.float32
    )


def general_shards(counts, library):
    own_block = normalize(counts, library)
    col_width = own_block.shape[1]
    cell_groups = lax.axis_size("cells")
    gene_total = col_width * lax.axis_size("genes")
    row_width = gene_total // cell_groups
    total_cells = float(counts.shape[0] * cell_groups)
    widened = own_block.astype(jnp.float32)
    local_sums = jnp.sum(widened, axis=0)
    local_squares = jnp.sum(widened * widened, axis=0)
    block_sums, block_squares = lax.psum((local_sums, local_squares), "cells")
    gene_sums, gene_squares = (
        lax.all_gather(block_sums, "genes", axis=0, tiled=True),
        lax.all_gather(block_squares, "genes", axis=0, tiled=True),
    )
    full_block = lax.all_gather(own_block, "genes", axis=1, tiled=True)
    gram_tile = lax.psum_scatter(
        cross_product(full_block, own_block), "cells", scatter_dimension=0, tiled=True
    )
    means = gene_sums / total_cells
    variances = gene_squares / total_cells - means * means
    scales = lax.rsqrt(variances + 1e-05)
    row_first = lax.axis_index("cells") * row_width
    col_first = lax.axis_index("genes") * col_width
    row_means = lax.dynamic_slice_in_dim(means, row_first, row_width, 0)
    col_means = lax.dynamic_slice_in_dim(means, col_first, col_width, 0)
    row_scales = lax.dynamic_slice_in_dim(scales, row_first, row_width, 0)
    col_scales = lax.dynamic_slice_in_dim(scales, col_first, col_width, 0)
    correlation = (
        (gram_tile / total_cells - row_means[:, None] * col_means[None, :])
        * row_scales[:, None]
        * col_scales[None, :]
    )
    powered = correlation**6
    row_index = row_first + jnp.arange(row_width, dtype=jnp.int32)[:, None]
    col_index = col_first + jnp.arange(col_width, dtype=jnp.int32)[None, :]
    adjacency = jnp.where(row_index == col_index, jnp.float32(0.0), powered)
    connectivity = lax.psum(jnp.sum(adjacency, axis=1), "genes")
    return (adjacency, connectivity)


def encode(x):
    return (x * jnp.abs(x) * (x * x)).astype(jnp.bfloat16)


def decode(y):
    y = y.astype(jnp.float32)
    root = lax.rsqrt(lax.rsqrt(jnp.abs(y)))
    return jnp.where(y < 0, -root, root)


def plain(left, right):
    return jnp.dot(left, right, preferred_element_type=jnp.float32)


def put_tiles(product, sums, s_ref, blk, rst, cst, cells, total, outs):
    odd = s_ref[CHIP] % 2
    row_side = jnp.concatenate([rst, jnp.broadcast_to(sums(rst), rst.shape)]).T
    mr, sr = row_side[:, 0:1], row_side[:, 1:2] * (1.0 / total)
    sx = row_side[:, rst.shape[0] : rst.shape[0] + 1]
    half = sr.shape[0]
    t = half // 2
    base = s_ref[CORE] ^ (s_ref[CHIP] // 2)
    for jj in range(2):
        first = pl.multiple_of((base ^ jj) * half, half)
        stat = cst(first, half)
        mc, sc = stat[0:1], stat[1:2]
        rest = sums(stat) - cells * mc
        tiles = [[None, None], [None, None]]
        for c in range(2):
            lanes = slice(c * t, c * t + t)
            p = product(pl.multiple_of(first + c * t, t), t)
            p = (p - sx * mc[:, lanes] - mr * rest[:, lanes]) * sr * sc[:, lanes]
            tiles[0][c], tiles[1][c] = p[:t], p[t:]
        for b in range(2):
            for i in range(2):
                tile = jnp.where(odd == 0, tiles[i][i ^ b], tiles[i][1 - (i ^ b)])
                j = 2 * jj + b
                outs[j][blk, i] = encode(tile) if j else tile


def row_stats(s_ref, st, plane, half):
    return st[plane, :, pl.ds(pl.multiple_of(s_ref[CORE] * half, half), half)]


def column_stats(st, plane):
    return lambda first, n: st[plane, :, pl.ds(first, n)]


def diagonal_body(s_ref, xa, xb, y0, y1, st, *outs, total):
    half = xa.shape[0]
    n = y0.shape[0] // 2

    def product(first, w):
        lanes = pl.ds(first, w)
        return (
            plain(xa[:, :n], y0[:n, lanes])
            + plain(xa[:, n:], y1[:n, lanes])
            + plain(xb[:, :n], y0[n:, lanes])
            + plain(xb[:, n:], y1[n:, lanes])
        )

    put_tiles(
        product, lambda v: v[2:3] + v[3:4], s_ref, 0,
        row_stats(s_ref, st, 0, half), column_stats(st, 0), 4.0 * n, total, outs,
    )


def near_body(s_ref, xa, xb, y0, y1, st, *outs, total):
    half = xa.shape[0]
    n = y0.shape[0] // 2
    for blk, x in enumerate((xa, xb)):
        cells = slice(blk * n, blk * n + n)

        def product(first, w):
            lanes = pl.ds(first, w)
            return plain(x[:, :n], y0[cells, lanes]) + plain(x[:, n:], y1[cells, lanes])

        put_tiles(
            product, lambda v: v[2 + blk : 3 + blk], s_ref, blk,
            row_stats(s_ref, st, s_ref[LOWER + blk], half), column_stats(st, 0),
            2.0 * n, total, outs,
        )


def pick_far(s_ref, xa, xb, xs):
    @pl.when(s_ref[LOW] == 0)
    def _():
        xs[...] = xa[...]

    @pl.when(s_ref[LOW] == 1)
    def _():
        xs[...] = xb[...]


def put_far(s_ref, product, st, plane, outs, cells, half, total):
    put_tiles(
        product, lambda v: jnp.where(s_ref[LOW] == 0, v[2:3], v[3:4]), s_ref, 0,
        row_stats(s_ref, st, 2, half), column_stats(st, plane), cells, total, outs,
    )


def far_body(s_ref, xa, xb, y0, y1, st, *refs, total):
    xs, outs = refs[-1], refs[:-1]
    half = xa.shape[0]
    n = y0.shape[0] // 2
    pick_far(s_ref, xa, xb, xs)
    cells = pl.ds(pl.multiple_of(s_ref[LOW] * n, n), n)

    def product(first, w):
        lanes = pl.ds(first, w)
        return plain(xs[:, :n], y0[cells, lanes]) + plain(xs[:, n:], y1[cells, lanes])

    put_far(s_ref, product, st, 0, outs, 2.0 * n, half, total)


def ends_body(s_ref, xa, xb, na, nb, st, *refs, total):
    xs, ys, outs = refs[-2], refs[-1], refs[:-2]
    half = xa.shape[0]
    n = na.shape[0] // 2
    pick_far(s_ref, xa, xb, xs)

    @pl.when(s_ref[CORE] == 0)
    def _():
        ys[:, :half] = na[...]
        ys[:n, half:] = nb[n:]
        ys[n:, half:] = nb[:n]

    @pl.when(s_ref[CORE] == 1)
    def _():
        ys[:, half:] = na[...]
        ys[:n, :half] = nb[n:]
        ys[n:, :half] = nb[:n]

    put_far(
        s_ref, lambda first, w: plain(xs[...], ys[:, pl.ds(first, w)]), st, 1, outs,
        2.0 * n, half, total,
    )


CHIP, CORE, PLANE, PLANES, LOW, LOWER, _, SHIFT, EARLY = range(9)


def turn_body(s_ref, own, r1, r2, r3, *outs, turns, keeps):
    odd = s_ref[CHIP] % 2
    t_ref, rest = outs[0], outs[1:]
    for n in range(own.shape[0]):
        for i in range(2):
            v = own[n, i] + decode(r1[n, i]) + decode(r2[n, i]) + decode(r3[n, i])
            t_ref[n, i] = v
            if keeps[n] is not None:
                rest[keeps[n]][i] = encode(v)
            if turns[n] is not None:
                w = encode(v.T)
                dst = rest[turns[n]]

                @pl.when(odd == 0)
                def _():
                    dst[i] = w

                @pl.when(odd == 1)
                def _():
                    dst[1 - i] = w


def power(v):
    v2 = v * v
    return v2 * v2 * v2


def put_slot(outs, where, i, value):
    for j, o in enumerate(outs):

        @pl.when(where == j)
        def _():
            o[i] = value


def row_total(v):
    return jnp.sum(v.T, axis=0, keepdims=True)


def early_body(s_ref, t0, t1, ru, rd, *refs):
    outs, sums = refs[:-1], refs[-1]
    k, g = s_ref[CHIP], s_ref[PLANE]
    n = t0.shape[-1]
    sums[...] = jnp.zeros_like(sums)
    for i in range(2):
        lanes = slice(i * n, i * n + n)
        own = power(t0[0, i])
        same = lax.broadcasted_iota(jnp.int32, (n, n), 0) == lax.broadcasted_iota(
            jnp.int32, (n, n), 1
        )
        own = jnp.where(same & (k == 0), 0.0, own)
        put_slot(outs, g ^ k, i, own.astype(jnp.bfloat16))
        sums[pl.ds(g, 1), lanes] = row_total(own)
        low = power(t1[0, i] + decode(ru[i]))
        high = power(t1[1, i] + decode(rd[i]))

        @pl.when(g > 0)
        def _():
            put_slot(outs, (g - 1) ^ k, i, low.astype(jnp.bfloat16))
            sums[pl.ds(g - 1, 1), lanes] = row_total(low)

        @pl.when(g < s_ref[PLANES] - 1)
        def _():
            put_slot(outs, (g + 1) ^ k, i, high.astype(jnp.bfloat16))
            sums[pl.ds(g + 1, 1), lanes] = row_total(high)


def late_body(s_ref, t2, r2, rf, rn, before, *refs):
    outs, sums = refs[:-1], refs[-1]
    k, g = s_ref[CHIP], s_ref[PLANE]
    n = t2.shape[-1]
    outer = (g == 0) | (g == s_ref[PLANES] - 1)
    sums[...] = before[...]
    for i in range(2):
        lanes = slice(i * n, i * n + n)
        two = power(t2[0, i] + decode(r2[i]))
        put_slot(outs, g ^ 2 ^ k, i, two.astype(jnp.bfloat16))
        sums[pl.ds(g ^ 2, 1), lanes] = row_total(two)

        @pl.when(outer)
        def _():
            three = power(decode(rf[i]) + decode(rn[i]))
            put_slot(outs, g ^ 3 ^ k, i, three.astype(jnp.bfloat16))
            sums[pl.ds(g ^ 3, 1), lanes] = row_total(three)


def place_body(s_ref, e0, e1, e2, e3, l0, l1, l2, l3, out_ref):
    x = s_ref[SHIFT]
    is_early = s_ref[EARLY]
    early, late = (e0, e1, e2, e3), (l0, l1, l2, l3)
    t = e0.shape[-1]

    def place(tiles):
        for i in range(2):
            for c in range(4):
                v = tiles[c ^ i][i]
                for m in range(1, 4):
                    v = jnp.where(x == m, tiles[c ^ i ^ m][i], v)
                out_ref[i * t : i * t + t, c * t : c * t + t] = v.astype(jnp.float32)

    @pl.when(is_early == 1)
    def _():
        place(early)

    @pl.when(is_early == 0)
    def _():
        place(late)


def pay_body(s_ref, a, *refs):
    out_a, out_b, out_n = refs[-3:]
    n = a.shape[0] // 2
    out_a[...] = a[:n].T
    out_b[...] = a[n:].T
    first = pl.multiple_of(jnp.where(s_ref[PLANE] == 0, n, 0), n)
    out_n[...] = a[pl.ds(first, n)]


def hold_body(a, out):
    out[...] = a[...]


def limit(mib):
    return pltpu.CompilerParams(vmem_limit_bytes=mib * 1024 * 1024)


def whole():
    return pl.BlockSpec(memory_space=pltpu.VMEM)


def scalars():
    return pl.BlockSpec(memory_space=pltpu.SMEM)


def folded_shards(counts, library):
    rows, width = counts.shape
    n_cells = lax.axis_size("cells")
    n_genes = lax.axis_size("genes")
    cores = n_cells // n_genes
    total = float(rows * n_cells)
    half_cells = rows // 2
    half = width // cores
    tile = half // 2
    g = lax.axis_index("genes")
    c = lax.axis_index("cells")
    k, h = c // cores, c % cores

    def perm(f):
        pairs = []
        for ci in range(n_cells):
            for gi in range(n_genes):
                d = f(ci // cores, ci % cores, gi)
                if d is not None and 0 <= d[2] < n_genes:
                    pairs.append((ci * n_genes + gi, (d[0] * cores + d[1]) * n_genes + d[2]))
        return pairs

    def send(x, f):
        return lax.ppermute(x, AXES, perm(f))

    flip = lambda k, h, g: (k, h ^ 1, g)
    bf16, f32 = jnp.bfloat16, jnp.float32
    shape = jax.ShapeDtypeStruct

    last = n_genes - 1
    own = normalize(counts, library)
    oth = send(own, flip)
    info = jnp.stack(
        [
            k,
            h,
            g,
            jnp.int32(n_genes),
            (g < n_genes // 2).astype(jnp.int32),
            jnp.where(g > 0, g ^ (g - 1), 0),
            jnp.where(g < last, g ^ (g + 1), 0),
            (2 * h) ^ k,
            (jnp.abs(k - g) <= 1).astype(jnp.int32),
        ]
    ).astype(jnp.int32)

    pay_in = pl.BlockSpec((rows, half), lambda i, sc: (0, sc[CORE]))
    pay_shapes = [shape((half, rows), bf16)] * 2 + [shape((rows, half), bf16)]

    def turn_payload(block, part, before):
        return pl.pallas_call(
            pay_body,
            grid_spec=pltpu.PrefetchScalarGridSpec(
                num_scalar_prefetch=1,
                grid=(1,),
                in_specs=[pay_in] + [pl.BlockSpec(memory_space=pl.ANY)] * len(before),
                out_specs=[pl.BlockSpec((half, half_cells), lambda i, sc: (0, part))] * 2
                + [pl.BlockSpec((half_cells, half), lambda i, sc: (part, 0))],
            ),
            out_shape=pay_shapes,
            input_output_aliases={2 + n: n for n in range(len(before))},
            compiler_params=limit(8),
            name="turn_payload",
        )(info, block, *before)

    pay_a, pay_b, end = turn_payload(oth, 1, turn_payload(own, 0, []))
    up1 = send(pay_a, lambda k, h, g: (k, h, g + 1))
    dn1 = send(pay_b, lambda k, h, g: (k, h, g - 1))
    widened = own.astype(f32)
    halves = jnp.sum(widened.reshape(2, half_cells, width), axis=1)
    squares = jnp.sum(widened * widened, axis=0)
    local = jnp.concatenate([halves, squares[None]])
    chip = local + send(local, flip)
    chip_halves = chip[:2]
    pair = jnp.stack([chip[0] + chip[1], chip[2]])
    around = [send(pair, lambda k, h, g, j=j: (k ^ j, h, g)) for j in (1, 2, 3)]
    sums = (pair + around[0]) + (around[1] + around[2])
    means = sums[0] / total
    variances = sums[1] / total - means * means
    mine = jnp.concatenate(
        [means[None], lax.rsqrt(variances + 1e-05)[None], chip_halves, jnp.zeros((4, width), f32)]
    )
    afar = [send(mine, lambda k, h, g, d=d: (k, h, g ^ d)) for d in (1, 2, 3)]
    own_stats = mine[None]
    stats = jnp.stack([mine] + afar)
    near = send(
        end, lambda k, h, g: (k, h, 1) if g == 0 else ((k, h, g - 1) if g == last else None)
    )

    oth = pl.pallas_call(
        hold_body,
        in_specs=[whole()],
        out_specs=whole(),
        out_shape=shape(oth.shape, bf16),
        compiler_params=limit(8),
        name="hold",
    )(oth)

    def blocks(body, n, scratch, *operands):
        return pl.pallas_call(
            functools.partial(body, total=total),
            in_specs=[scalars()] + [whole()] * len(operands),
            out_specs=[whole()] * 4,
            out_shape=[shape((n, 2, tile, tile), f32)]
            + [shape((n, 2, tile, tile), bf16)] * 3,
            scratch_shapes=[pltpu.VMEM(v, bf16) for v in scratch],
            compiler_params=limit(24),
            name="partial_blocks",
        )(info, *operands)

    up2 = send(up1, lambda k, h, g: (k, h, g + 1) if g > 0 else None)
    dn2 = send(dn1, lambda k, h, g: (k, h, g - 1) if g < last else None)
    near_other = send(near, flip)
    kept = (half, rows)
    w0 = blocks(diagonal_body, 1, [], pay_a, pay_b, own, oth, own_stats)
    w1 = blocks(near_body, 2, [], up1, dn1, own, oth, stats)
    w2 = blocks(far_body, 1, [kept], up2, dn2, own, oth, stats)
    w3 = blocks(ends_body, 1, [kept, (rows, width)], up2, dn2, near, near_other, stats)

    def reduce_tiles(w):
        return [w[0]] + [send(w[j], lambda k, h, g, j=j: (k ^ j, h, g)) for j in (1, 2, 3)]

    small = shape((2, tile, tile), bf16)

    def turn(parts, turns, keeps):
        n = parts[0].shape[0]
        n_out = sum(v is not None for v in turns + keeps)
        return pl.pallas_call(
            functools.partial(turn_body, turns=turns, keeps=keeps),
            in_specs=[scalars()] + [whole()] * 4,
            out_specs=[whole()] * (1 + n_out),
            out_shape=[shape((n, 2, tile, tile), f32)] + [small] * n_out,
            compiler_params=limit(12),
            name="sum_tiles",
        )(info, *parts)

    (t0,) = turn(reduce_tiles(w0), [None], [None])
    t1, e_up, e_dn = turn(reduce_tiles(w1), [0, 1], [None, None])
    t2, e_two = turn(reduce_tiles(w2), [0], [None])
    _, e_three, k_three = turn(reduce_tiles(w3), [0], [1])

    side = lambda f: (lambda k, h, g: (k, h ^ (k // 2), f(g)) if f(g) is not None else None)
    rd = send(e_up, side(lambda g: g - 1))
    ru = send(e_dn, side(lambda g: g + 1))
    r2 = send(e_two, side(lambda g: g ^ 2))
    inner = lambda g: 0 < g < last
    r3f = send(e_three, side(lambda g: (g ^ 2) if inner(g) else None))
    r3n = send(k_three, lambda k, h, g: (k, h, g ^ 1) if inner(g) else None)

    def finish(body, *operands):
        return pl.pallas_call(
            body,
            in_specs=[scalars()] + [whole()] * len(operands),
            out_specs=[whole()] * 5,
            out_shape=[small] * 4 + [shape((n_genes, half), f32)],
            compiler_params=limit(10),
            name="finish_tiles",
        )(info, *operands)

    *early, early_sums = finish(early_body, t0, t1, ru, rd)
    *late, tile_sums = finish(late_body, t2, r2, r3f, r3n, early_sums)

    is_early = lambda q, g: -1 <= q - g <= 1
    got_early, got_late = [early[0]], [late[0]]
    for j in range(1, 4):
        got_early.append(
            send(early[j], lambda k, h, g, j=j: (k ^ j, h, g) if is_early(k ^ j, g) else None)
        )
        got_late.append(
            send(late[j], lambda k, h, g, j=j: (k ^ j, h, g) if not is_early(k ^ j, g) else None)
        )
    adjacency = pl.pallas_call(
        place_body,
        in_specs=[scalars()] + [whole()] * 8,
        out_specs=whole(),
        out_shape=shape((half, width), f32),
        compiler_params=limit(12),
        name="place_tiles",
    )(info, *got_early, *got_late)
    over = [send(tile_sums, lambda k, h, g, d=d: (k, h, g ^ d)) for d in (1, 2, 3)]
    chip_sums = (tile_sums + over[0]) + (over[1] + over[2])

    def rows_of(q):
        return lax.dynamic_index_in_dim(chip_sums, q, 0, keepdims=False)

    inside = [rows_of(k)] + [
        send(rows_of(k ^ j), lambda k, h, g, j=j: (k ^ j, h, g)) for j in (1, 2, 3)
    ]
    connectivity = (inside[0] + inside[1]) + (inside[2] + inside[3])
    return (adjacency, connectivity)


def folded(counts, library):
    return folded_shards(counts, library)


def solution(mesh):
    cells, genes = mesh.shape["cells"], mesh.shape["genes"]
    folds = genes == 4 and cells == 2 * genes
    return jax.shard_map(
        folded if folds else general_shards,
        mesh=mesh,
        in_specs=(P("cells", "genes"), P("cells")),
        out_specs=(P("cells", "genes"), P("cells")),
        check_vma=False,
    )
```

```python
import functools

import jax
import jax.numpy as jnp
from jax import lax
from jax.experimental import pallas as pl
from jax.experimental.pallas import tpu as pltpu
from jax.sharding import PartitionSpec as P


AXES = ("cells", "genes")


def normalize(counts, library):
    factor = 10000.0 / library.astype(jnp.float32)
    return jnp.log1p(counts.astype(jnp.float32) * factor[:, None]).astype(jnp.bfloat16)


def cross_product(left, right):
    return lax.dot_general(
        left, right, (((0,), (0,)), ((), ())), preferred_element_type=jnp.float32
    )


def general_shards(counts, library):
    own_block = normalize(counts, library)
    col_width = own_block.shape[1]
    cell_groups = lax.axis_size("cells")
    gene_total = col_width * lax.axis_size("genes")
    row_width = gene_total // cell_groups
    total_cells = float(counts.shape[0] * cell_groups)
    widened = own_block.astype(jnp.float32)
    local_sums = jnp.sum(widened, axis=0)
    local_squares = jnp.sum(widened * widened, axis=0)
    block_sums, block_squares = lax.psum((local_sums, local_squares), "cells")
    gene_sums, gene_squares = (
        lax.all_gather(block_sums, "genes", axis=0, tiled=True),
        lax.all_gather(block_squares, "genes", axis=0, tiled=True),
    )
    full_block = lax.all_gather(own_block, "genes", axis=1, tiled=True)
    gram_tile = lax.psum_scatter(
        cross_product(full_block, own_block), "cells", scatter_dimension=0, tiled=True
    )
    means = gene_sums / total_cells
    variances = gene_squares / total_cells - means * means
    scales = lax.rsqrt(variances + 1e-05)
    row_first = lax.axis_index("cells") * row_width
    col_first = lax.axis_index("genes") * col_width
    row_means = lax.dynamic_slice_in_dim(means, row_first, row_width, 0)
    col_means = lax.dynamic_slice_in_dim(means, col_first, col_width, 0)
    row_scales = lax.dynamic_slice_in_dim(scales, row_first, row_width, 0)
    col_scales = lax.dynamic_slice_in_dim(scales, col_first, col_width, 0)
    correlation = (
        (gram_tile / total_cells - row_means[:, None] * col_means[None, :])
        * row_scales[:, None]
        * col_scales[None, :]
    )
    powered = correlation**6
    row_index = row_first + jnp.arange(row_width, dtype=jnp.int32)[:, None]
    col_index = col_first + jnp.arange(col_width, dtype=jnp.int32)[None, :]
    adjacency = jnp.where(row_index == col_index, jnp.float32(0.0), powered)
    connectivity = lax.psum(jnp.sum(adjacency, axis=1), "genes")
    return (adjacency, connectivity)


def encode(x):
    return (x * jnp.abs(x) * (x * x)).astype(jnp.bfloat16)


def decode(y):
    y = y.astype(jnp.float32)
    root = lax.rsqrt(lax.rsqrt(jnp.abs(y)))
    return jnp.where(y < 0, -root, root)


def plain(left, right):
    return jnp.dot(left, right, preferred_element_type=jnp.float32)


def put_tiles(product, sums, s_ref, blk, rst, cst, cells, total, outs):
    odd = s_ref[CHIP] % 2
    row_side = jnp.concatenate([rst, jnp.broadcast_to(sums(rst), rst.shape)]).T
    mr, sr = row_side[:, 0:1], row_side[:, 1:2] * (1.0 / total)
    sx = row_side[:, rst.shape[0] : rst.shape[0] + 1]
    half = sr.shape[0]
    t = half // 2
    base = s_ref[CORE] ^ (s_ref[CHIP] // 2)
    for jj in range(2):
        first = pl.multiple_of((base ^ jj) * half, half)
        stat = cst(first, half)
        mc, sc = stat[0:1], stat[1:2]
        rest = sums(stat) - cells * mc
        tiles = [[None, None], [None, None]]
        for c in range(2):
            lanes = slice(c * t, c * t + t)
            p = product(pl.multiple_of(first + c * t, t), t)
            p = (p - sx * mc[:, lanes] - mr * rest[:, lanes]) * sr * sc[:, lanes]
            tiles[0][c], tiles[1][c] = p[:t], p[t:]
        for b in range(2):
            for i in range(2):
                tile = jnp.where(odd == 0, tiles[i][i ^ b], tiles[i][1 - (i ^ b)])
                j = 2 * jj + b
                outs[j][blk, i] = encode(tile) if j else tile


def row_stats(s_ref, st, plane, half):
    return st[plane, :, pl.ds(pl.multiple_of(s_ref[CORE] * half, half), half)]


def column_stats(st, plane):
    return lambda first, n: st[plane, :, pl.ds(first, n)]


def diagonal_body(s_ref, xa, xb, y0, y1, st, *outs, total):
    half = xa.shape[0]
    n = y0.shape[0] // 2

    def product(first, w):
        lanes = pl.ds(first, w)
        return (
            plain(xa[:, :n], y0[:n, lanes])
            + plain(xa[:, n:], y1[:n, lanes])
            + plain(xb[:, :n], y0[n:, lanes])
            + plain(xb[:, n:], y1[n:, lanes])
        )

    put_tiles(
        product, lambda v: v[2:3] + v[3:4], s_ref, 0,
        row_stats(s_ref, st, 0, half), column_stats(st, 0), 4.0 * n, total, outs,
    )


def near_body(s_ref, xa, xb, y0, y1, st, *outs, total):
    half = xa.shape[0]
    n = y0.shape[0] // 2
    for blk, x in enumerate((xa, xb)):
        cells = slice(blk * n, blk * n + n)

        def product(first, w):
            lanes = pl.ds(first, w)
            return plain(x[:, :n], y0[cells, lanes]) + plain(x[:, n:], y1[cells, lanes])

        put_tiles(
            product, lambda v: v[2 + blk : 3 + blk], s_ref, blk,
            row_stats(s_ref, st, s_ref[LOWER + blk], half), column_stats(st, 0),
            2.0 * n, total, outs,
        )


def pick_far(s_ref, xa, xb, xs):
    @pl.when(s_ref[LOW] == 0)
    def _():
        xs[...] = xa[...]

    @pl.when(s_ref[LOW] == 1)
    def _():
        xs[...] = xb[...]


def put_far(s_ref, product, st, plane, outs, cells, half, total):
    put_tiles(
        product, lambda v: jnp.where(s_ref[LOW] == 0, v[2:3], v[3:4]), s_ref, 0,
        row_stats(s_ref, st, 2, half), column_stats(st, plane), cells, total, outs,
    )


def far_body(s_ref, xa, xb, y0, y1, st, first_tiles, *refs, total):
    xs, outs = refs[-1], refs[:-1]
    half = xa.shape[0]
    n = y0.shape[0] // 2
    pick_far(s_ref, xa, xb, xs)
    cells = pl.ds(pl.multiple_of(s_ref[LOW] * n, n), n)

    def product(first, w):
        lanes = pl.ds(first, w)
        return plain(xs[:, :n], y0[cells, lanes]) + plain(xs[:, n:], y1[cells, lanes])

    put_far(s_ref, product, st, 0, outs, 2.0 * n, half, total)


def ends_body(s_ref, xa, xb, na, nb, st, *refs, total):
    xs, ys, outs = refs[-2], refs[-1], refs[:-2]
    half = xa.shape[0]
    n = na.shape[0] // 2
    pick_far(s_ref, xa, xb, xs)

    @pl.when(s_ref[CORE] == 0)
    def _():
        ys[:, :half] = na[...]
        ys[:n, half:] = nb[n:]
        ys[n:, half:] = nb[:n]

    @pl.when(s_ref[CORE] == 1)
    def _():
        ys[:, half:] = na[...]
        ys[:n, :half] = nb[n:]
        ys[n:, :half] = nb[:n]

    put_far(
        s_ref, lambda first, w: plain(xs[...], ys[:, pl.ds(first, w)]), st, 1, outs,
        2.0 * n, half, total,
    )


CHIP, CORE, PLANE, PLANES, LOW, LOWER, _, SHIFT, _ = range(9)


def turn_body(s_ref, own, r1, r2, r3, *outs, turns, keeps):
    odd = s_ref[CHIP] % 2
    t_ref, rest = outs[0], outs[1:]
    for n in range(own.shape[0]):
        for i in range(2):
            v = own[n, i] + decode(r1[n, i]) + decode(r2[n, i]) + decode(r3[n, i])
            t_ref[n, i] = v
            if keeps[n] is not None:
                rest[keeps[n]][i] = encode(v)
            if turns[n] is not None:
                w = encode(v.T)
                dst = rest[turns[n]]

                @pl.when(odd == 0)
                def _():
                    dst[i] = w

                @pl.when(odd == 1)
                def _():
                    dst[1 - i] = w


def power(v):
    v2 = v * v
    return v2 * v2 * v2


def put_slot(outs, where, i, value):
    for j, o in enumerate(outs):

        @pl.when(where == j)
        def _():
            o[i] = value


def column_total(v):
    return jnp.sum(v, axis=0, keepdims=True)


def column_place(k, i, n):
    return pl.ds(pl.multiple_of((i ^ (k % 2)) * n, n), n)


def early_body(s_ref, t0, t1, ru, rd, *refs):
    outs, sums = refs[:-1], refs[-1]
    k, g = s_ref[CHIP], s_ref[PLANE]
    n = t0.shape[-1]
    for i in range(2):
        own = power(t0[0, i])
        same = lax.broadcasted_iota(jnp.int32, (n, n), 0) == lax.broadcasted_iota(
            jnp.int32, (n, n), 1
        )
        own = jnp.where(same & (k == 0), 0.0, own)
        low = power(t1[0, i] + decode(ru[i]))
        high = power(t1[1, i] + decode(rd[i]))
        has_low, has_high = g > 0, g < s_ref[PLANES] - 1
        put_slot(outs, g ^ k, i, own.astype(jnp.bfloat16))
        put_slot(outs, jnp.where(has_low, (g - 1) ^ k, -1), i, low.astype(jnp.bfloat16))
        put_slot(outs, jnp.where(has_high, (g + 1) ^ k, -1), i, high.astype(jnp.bfloat16))
        sums[0:1, column_place(k, i, n)] = (
            column_total(own)
            + jnp.where(has_low, column_total(low), 0.0)
            + jnp.where(has_high, column_total(high), 0.0)
        )


def late_body(s_ref, t2, r2, rf, rn, before, *refs):
    outs, sums = refs[4:-1], refs[-1]
    k, g = s_ref[CHIP], s_ref[PLANE]
    n = t2.shape[-1]
    outer = (g == 0) | (g == s_ref[PLANES] - 1)
    for i in range(2):
        at = column_place(k, i, n)
        two = power(t2[0, i] + decode(r2[i]))
        three = power(decode(rf[i]) + decode(rn[i]))
        put_slot(outs, g ^ 2 ^ k, i, two.astype(jnp.bfloat16))
        put_slot(outs, jnp.where(outer, g ^ 3 ^ k, -1), i, three.astype(jnp.bfloat16))
        sums[0:1, at] = (
            before[0:1, at] + column_total(two) + jnp.where(outer, column_total(three), 0.0)
        )


def place_body(s_ref, t0, t1, t2, t3, out_ref):
    x = s_ref[SHIFT]
    tiles = (t0, t1, t2, t3)
    t = t0.shape[-1]
    for i in range(2):
        for c in range(4):
            v = tiles[c ^ i][i]
            for m in range(1, 4):
                v = jnp.where(x == m, tiles[c ^ i ^ m][i], v)
            out_ref[i * t : i * t + t, c * t : c * t + t] = v.astype(jnp.float32)


def pay_body(s_ref, a, *refs):
    out_a, out_b, out_n = refs[-3:]
    n = a.shape[0] // 2
    out_a[...] = a[:n].T
    out_b[...] = a[n:].T
    first = pl.multiple_of(jnp.where(s_ref[PLANE] == 0, n, 0), n)
    out_n[...] = a[pl.ds(first, n)]


def hold_body(a, sums, out, chip):
    n = a.shape[0] // 2
    out[...] = a[...]
    wide = a[...].astype(jnp.float32)
    chip[0:1] = sums[0:1] + jnp.sum(wide[:n], axis=0, keepdims=True)
    chip[1:2] = sums[1:2] + jnp.sum(wide[n:], axis=0, keepdims=True)
    chip[2:3] = sums[2:3] + jnp.sum(wide * wide, axis=0, keepdims=True)


def limit(mib):
    return pltpu.CompilerParams(vmem_limit_bytes=mib * 1024 * 1024)


def whole():
    return pl.BlockSpec(memory_space=pltpu.VMEM)


def scalars():
    return pl.BlockSpec(memory_space=pltpu.SMEM)


def folded_shards(counts, library):
    rows, width = counts.shape
    n_cells = lax.axis_size("cells")
    n_genes = lax.axis_size("genes")
    cores = n_cells // n_genes
    total = float(rows * n_cells)
    half_cells = rows // 2
    half = width // cores
    tile = half // 2
    g = lax.axis_index("genes")
    c = lax.axis_index("cells")
    k, h = c // cores, c % cores

    def perm(f):
        pairs = []
        for ci in range(n_cells):
            for gi in range(n_genes):
                d = f(ci // cores, ci % cores, gi)
                if d is not None and 0 <= d[2] < n_genes:
                    pairs.append((ci * n_genes + gi, (d[0] * cores + d[1]) * n_genes + d[2]))
        return pairs

    def send(x, f):
        return lax.ppermute(x, AXES, perm(f))

    flip = lambda k, h, g: (k, h ^ 1, g)
    bf16, f32 = jnp.bfloat16, jnp.float32
    shape = jax.ShapeDtypeStruct

    last = n_genes - 1
    info = jnp.stack(
        [
            k,
            h,
            g,
            jnp.int32(n_genes),
            (g < n_genes // 2).astype(jnp.int32),
            jnp.where(g > 0, g ^ (g - 1), 0),
            jnp.where(g < last, g ^ (g + 1), 0),
            (2 * h) ^ k,
            (jnp.abs(k - g) <= 1).astype(jnp.int32),
        ]
    ).astype(jnp.int32)

    own = normalize(counts, library)
    oth = send(own, flip)
    pay_in = pl.BlockSpec((rows, half), lambda i, sc: (0, sc[CORE]))
    pay_shapes = [shape((half, rows), bf16)] * 2 + [shape((rows, half), bf16)]

    def turn_payload(block, part, before):
        return pl.pallas_call(
            pay_body,
            grid_spec=pltpu.PrefetchScalarGridSpec(
                num_scalar_prefetch=1,
                grid=(1,),
                in_specs=[pay_in] + [pl.BlockSpec(memory_space=pl.ANY)] * len(before),
                out_specs=[pl.BlockSpec((half, half_cells), lambda i, sc: (0, part))] * 2
                + [pl.BlockSpec((half_cells, half), lambda i, sc: (part, 0))],
            ),
            out_shape=pay_shapes,
            input_output_aliases={2 + n: n for n in range(len(before))},
            compiler_params=limit(8),
            name="turn_payload",
        )(info, block, *before)

    pay_a, pay_b, end = turn_payload(oth, 1, turn_payload(own, 0, []))
    up1 = send(pay_a, lambda k, h, g: (k, h, g + 1))
    dn1 = send(pay_b, lambda k, h, g: (k, h, g - 1))
    widened = own.astype(f32)
    halves = jnp.sum(widened.reshape(2, half_cells, width), axis=1)
    squares = jnp.sum(widened * widened, axis=0)
    oth, chip = pl.pallas_call(
        hold_body,
        in_specs=[whole()] * 2,
        out_specs=[whole()] * 2,
        out_shape=[shape(oth.shape, bf16), shape((3, width), f32)],
        compiler_params=limit(14),
        name="hold",
    )(oth, jnp.concatenate([halves, squares[None]]))
    chip_halves = chip[:2]
    around = [send(chip, lambda k, h, g, j=j: (k ^ j, h, g)) for j in (1, 2, 3)]
    every = (chip + around[0]) + (around[1] + around[2])
    sums = [every[0] + every[1], every[2]]
    means = sums[0] / total
    variances = sums[1] / total - means * means
    packed = jnp.concatenate(
        [means[None], lax.rsqrt(variances + 1e-05)[None], chip_halves, jnp.zeros((4, width), f32)]
    )
    afar = [send(packed, lambda k, h, g, d=d: (k, h, g ^ d)) for d in (1, 2, 3)]
    own_stats = packed[None]
    stats = jnp.stack([packed] + afar)
    near = send(
        end, lambda k, h, g: (k, h, 1) if g == 0 else ((k, h, g - 1) if g == last else None)
    )

    def blocks(body, n, scratch, *operands, behind=0):
        return pl.pallas_call(
            functools.partial(body, total=total),
            in_specs=[scalars()]
            + [whole()] * (len(operands) - behind)
            + [pl.BlockSpec(memory_space=pl.ANY)] * behind,
            out_specs=[whole()] * 4,
            out_shape=[shape((n, 2, tile, tile), f32)]
            + [shape((n, 2, tile, tile), bf16)] * 3,
            scratch_shapes=[pltpu.VMEM(v, bf16) for v in scratch],
            compiler_params=limit(24),
            name="partial_blocks",
        )(info, *operands)

    up2 = send(up1, lambda k, h, g: (k, h, g + 1) if g > 0 else None)
    dn2 = send(dn1, lambda k, h, g: (k, h, g - 1) if g < last else None)
    near_other = send(near, flip)
    kept = (half, rows)
    w0 = blocks(diagonal_body, 1, [], pay_a, pay_b, own, oth, own_stats)
    w1 = blocks(near_body, 2, [], up1, dn1, own, oth, stats)
    w3 = blocks(ends_body, 1, [kept, (rows, width)], up2, dn2, near, near_other, stats)

    def reduce_tiles(w):
        return [w[0]] + [send(w[j], lambda k, h, g, j=j: (k ^ j, h, g)) for j in (1, 2, 3)]

    small = shape((2, tile, tile), bf16)

    def turn(parts, turns, keeps):
        n = parts[0].shape[0]
        n_out = sum(v is not None for v in turns + keeps)
        return pl.pallas_call(
            functools.partial(turn_body, turns=turns, keeps=keeps),
            in_specs=[scalars()] + [whole()] * 4,
            out_specs=[whole()] * (1 + n_out),
            out_shape=[shape((n, 2, tile, tile), f32)] + [small] * n_out,
            compiler_params=limit(12),
            name="sum_tiles",
        )(info, *parts)

    (t0,) = turn(reduce_tiles(w0), [None], [None])
    w2 = blocks(far_body, 1, [kept], up2, dn2, own, oth, stats, t0, behind=1)
    t1, e_up, e_dn = turn(reduce_tiles(w1), [0, 1], [None, None])
    t2, e_two = turn(reduce_tiles(w2), [0], [None])
    _, e_three, k_three = turn(reduce_tiles(w3), [0], [1])

    side = lambda f: (lambda k, h, g: (k, h ^ (k // 2), f(g)) if f(g) is not None else None)
    rd = send(e_up, side(lambda g: g - 1))
    ru = send(e_dn, side(lambda g: g + 1))
    r2 = send(e_two, side(lambda g: g ^ 2))
    inner = lambda g: 0 < g < last
    r3f = send(e_three, side(lambda g: (g ^ 2) if inner(g) else None))
    r3n = send(k_three, lambda k, h, g: (k, h, g ^ 1) if inner(g) else None)

    def finish(body, *operands, over=0):
        return pl.pallas_call(
            body,
            in_specs=[scalars()] + [whole()] * len(operands),
            input_output_aliases={1 + len(operands) - over + n: n for n in range(over)},
            out_specs=[whole()] * 5,
            out_shape=[small] * 4 + [shape((1, half), f32)],
            compiler_params=limit(10),
            name="finish_tiles",
        )(info, *operands)

    *close, close_sums = finish(early_body, t0, t1, ru, rd)
    *tiles, tile_sums = finish(late_body, t2, r2, r3f, r3n, close_sums, *close, over=len(close))
    got = [tiles[0]] + [send(tiles[j], lambda k, h, g, j=j: (k ^ j, h, g)) for j in (1, 2, 3)]
    adjacency = pl.pallas_call(
        place_body,
        in_specs=[scalars()] + [whole()] * 4,
        out_specs=whole(),
        out_shape=shape((half, width), f32),
        compiler_params=limit(12),
        name="place_tiles",
    )(info, *got)
    sums = [send(tile_sums, lambda k, h, g, m=m: (g, h ^ (k // 2), k ^ m)) for m in range(4)]
    connectivity = ((sums[0] + sums[1]) + (sums[2] + sums[3])).reshape(half)
    return (adjacency, connectivity)


def folded(counts, library):
    return folded_shards(counts, library)


def solution(mesh):
    cells, genes = mesh.shape["cells"], mesh.shape["genes"]
    folds = genes == 4 and cells == 2 * genes
    return jax.shard_map(
        folded if folds else general_shards,
        mesh=mesh,
        in_specs=(P("cells", "genes"), P("cells")),
        out_specs=(P("cells", "genes"), P("cells")),
        check_vma=False,
    )
```

```python
import functools

import jax
import jax.numpy as jnp
from jax import lax
from jax.experimental import pallas as pl
from jax.experimental.pallas import tpu as pltpu
from jax.sharding import PartitionSpec as P


AXES = ("cells", "genes")


def normalize(counts, library):
    factor = 10000.0 / library.astype(jnp.float32)
    return jnp.log1p(counts.astype(jnp.float32) * factor[:, None]).astype(jnp.bfloat16)


def cross_product(left, right):
    return lax.dot_general(
        left, right, (((0,), (0,)), ((), ())), preferred_element_type=jnp.float32
    )


def general_shards(counts, library):
    own_block = normalize(counts, library)
    col_width = own_block.shape[1]
    cell_groups = lax.axis_size("cells")
    gene_total = col_width * lax.axis_size("genes")
    row_width = gene_total // cell_groups
    total_cells = float(counts.shape[0] * cell_groups)
    widened = own_block.astype(jnp.float32)
    local_sums = jnp.sum(widened, axis=0)
    local_squares = jnp.sum(widened * widened, axis=0)
    block_sums, block_squares = lax.psum((local_sums, local_squares), "cells")
    gene_sums, gene_squares = (
        lax.all_gather(block_sums, "genes", axis=0, tiled=True),
        lax.all_gather(block_squares, "genes", axis=0, tiled=True),
    )
    full_block = lax.all_gather(own_block, "genes", axis=1, tiled=True)
    gram_tile = lax.psum_scatter(
        cross_product(full_block, own_block), "cells", scatter_dimension=0, tiled=True
    )
    means = gene_sums / total_cells
    variances = gene_squares / total_cells - means * means
    scales = lax.rsqrt(variances + 1e-05)
    row_first = lax.axis_index("cells") * row_width
    col_first = lax.axis_index("genes") * col_width
    row_means = lax.dynamic_slice_in_dim(means, row_first, row_width, 0)
    col_means = lax.dynamic_slice_in_dim(means, col_first, col_width, 0)
    row_scales = lax.dynamic_slice_in_dim(scales, row_first, row_width, 0)
    col_scales = lax.dynamic_slice_in_dim(scales, col_first, col_width, 0)
    correlation = (
        (gram_tile / total_cells - row_means[:, None] * col_means[None, :])
        * row_scales[:, None]
        * col_scales[None, :]
    )
    powered = correlation**6
    row_index = row_first + jnp.arange(row_width, dtype=jnp.int32)[:, None]
    col_index = col_first + jnp.arange(col_width, dtype=jnp.int32)[None, :]
    adjacency = jnp.where(row_index == col_index, jnp.float32(0.0), powered)
    connectivity = lax.psum(jnp.sum(adjacency, axis=1), "genes")
    return (adjacency, connectivity)


def encode(x):
    return (x * jnp.abs(x) * (x * x)).astype(jnp.bfloat16)


def decode(y):
    y = y.astype(jnp.float32)
    root = lax.rsqrt(lax.rsqrt(jnp.abs(y)))
    return jnp.where(y < 0, -root, root)


def plain(left, right):
    return jnp.dot(left, right, preferred_element_type=jnp.float32)


def put_tiles(product, sums, s_ref, blk, rst, cst, cells, total, outs):
    odd = s_ref[CHIP] % 2
    row_side = jnp.concatenate([rst, jnp.broadcast_to(sums(rst), rst.shape)]).T
    mr, sr = row_side[:, 0:1], row_side[:, 1:2] * (1.0 / total)
    sx = row_side[:, rst.shape[0] : rst.shape[0] + 1]
    half = sr.shape[0]
    t = half // 2
    base = s_ref[CORE] ^ (s_ref[CHIP] // 2)
    for jj in range(2):
        first = pl.multiple_of((base ^ jj) * half, half)
        stat = cst(first, half)
        mc, sc = stat[0:1], stat[1:2]
        rest = sums(stat) - cells * mc
        tiles = [[None, None], [None, None]]
        for c in range(2):
            lanes = slice(c * t, c * t + t)
            p = product(pl.multiple_of(first + c * t, t), t)
            p = (p - sx * mc[:, lanes] - mr * rest[:, lanes]) * sr * sc[:, lanes]
            tiles[0][c], tiles[1][c] = p[:t], p[t:]
        for b in range(2):
            for i in range(2):
                tile = jnp.where(odd == 0, tiles[i][i ^ b], tiles[i][1 - (i ^ b)])
                j = 2 * jj + b
                outs[j][blk, i] = encode(tile) if j else tile


def row_stats(s_ref, st, plane, half):
    return st[plane, :, pl.ds(pl.multiple_of(s_ref[CORE] * half, half), half)]


def column_stats(st, plane):
    return lambda first, n: st[plane, :, pl.ds(first, n)]


def stacked(products):
    return jnp.concatenate(products, axis=0)


def diagonal_body(s_ref, a0, a1, b0, b1, y0, y1, st, *outs, total):
    half = 2 * a0.shape[0]
    n = y0.shape[0] // 2

    def product(first, w):
        lanes = pl.ds(first, w)
        return stacked(
            [
                plain(xa[:, :n], y0[:n, lanes])
                + plain(xa[:, n:], y1[:n, lanes])
                + plain(xb[:, :n], y0[n:, lanes])
                + plain(xb[:, n:], y1[n:, lanes])
                for xa, xb in ((a0, b0), (a1, b1))
            ]
        )

    put_tiles(
        product, lambda v: v[2:3] + v[3:4], s_ref, 0,
        row_stats(s_ref, st, 0, half), column_stats(st, 0), 4.0 * n, total, outs,
    )


def near_body(s_ref, a0, a1, b0, b1, y0, y1, st, *outs, total):
    half = 2 * a0.shape[0]
    n = y0.shape[0] // 2
    for blk, xs in enumerate(((a0, a1), (b0, b1))):
        cells = slice(blk * n, blk * n + n)

        def product(first, w):
            lanes = pl.ds(first, w)
            return stacked(
                [plain(x[:, :n], y0[cells, lanes]) + plain(x[:, n:], y1[cells, lanes]) for x in xs]
            )

        put_tiles(
            product, lambda v: v[2 + blk : 3 + blk], s_ref, blk,
            row_stats(s_ref, st, s_ref[LOWER + blk], half), column_stats(st, 0),
            2.0 * n, total, outs,
        )


def pick_far(s_ref, a0, a1, b0, b1, xs):
    t = a0.shape[0]

    @pl.when(s_ref[LOW] == 0)
    def _():
        xs[:t] = a0[...]
        xs[t:] = a1[...]

    @pl.when(s_ref[LOW] == 1)
    def _():
        xs[:t] = b0[...]
        xs[t:] = b1[...]


def put_far(s_ref, product, st, plane, outs, cells, half, total):
    put_tiles(
        product, lambda v: jnp.where(s_ref[LOW] == 0, v[2:3], v[3:4]), s_ref, 0,
        row_stats(s_ref, st, 2, half), column_stats(st, plane), cells, total, outs,
    )


def far_body(s_ref, a0, a1, b0, b1, y0, y1, st, *refs, total):
    xs, outs = refs[-1], refs[:-1]
    half = 2 * a0.shape[0]
    n = y0.shape[0] // 2
    pick_far(s_ref, a0, a1, b0, b1, xs)
    cells = pl.ds(pl.multiple_of(s_ref[LOW] * n, n), n)

    def product(first, w):
        lanes = pl.ds(first, w)
        return plain(xs[:, :n], y0[cells, lanes]) + plain(xs[:, n:], y1[cells, lanes])

    put_far(s_ref, product, st, 0, outs, 2.0 * n, half, total)


def ends_body(s_ref, a0, a1, b0, b1, na, nb, st, *refs, total):
    xs, ys, outs = refs[-2], refs[-1], refs[:-2]
    half = 2 * a0.shape[0]
    n = na.shape[0] // 2
    pick_far(s_ref, a0, a1, b0, b1, xs)

    @pl.when(s_ref[CORE] == 0)
    def _():
        ys[:, :half] = na[...]
        ys[:n, half:] = nb[n:]
        ys[n:, half:] = nb[:n]

    @pl.when(s_ref[CORE] == 1)
    def _():
        ys[:, half:] = na[...]
        ys[:n, :half] = nb[n:]
        ys[n:, :half] = nb[:n]

    put_far(
        s_ref, lambda first, w: plain(xs[...], ys[:, pl.ds(first, w)]), st, 1, outs,
        2.0 * n, half, total,
    )


CHIP, CORE, PLANE, PLANES, LOW, LOWER, _, SHIFT, _ = range(9)


def turn_body(s_ref, own, r1, r2, r3, *outs, turns, keeps):
    odd = s_ref[CHIP] % 2
    t_ref, rest = outs[0], outs[1:]
    for n in range(own.shape[0]):
        for i in range(2):
            v = own[n, i] + decode(r1[n, i]) + decode(r2[n, i]) + decode(r3[n, i])
            t_ref[n, i] = v
            if keeps[n] is not None:
                rest[keeps[n]][i] = encode(v)
            if turns[n] is not None:
                w = encode(v.T)
                dst = rest[turns[n]]

                @pl.when(odd == 0)
                def _():
                    dst[i] = w

                @pl.when(odd == 1)
                def _():
                    dst[1 - i] = w


def power(v):
    v2 = v * v
    return v2 * v2 * v2


def put_slot(outs, where, i, value):
    for j, o in enumerate(outs):

        @pl.when(where == j)
        def _():
            o[i] = value


def column_total(v):
    return jnp.sum(v, axis=0, keepdims=True)


def column_place(k, i, n):
    return pl.ds(pl.multiple_of((i ^ (k % 2)) * n, n), n)


def early_body(s_ref, t0, t1, ru, rd, *refs):
    outs, sums = refs[:-1], refs[-1]
    k, g = s_ref[CHIP], s_ref[PLANE]
    n = t0.shape[-1]
    for i in range(2):
        own = power(t0[0, i])
        same = lax.broadcasted_iota(jnp.int32, (n, n), 0) == lax.broadcasted_iota(
            jnp.int32, (n, n), 1
        )
        own = jnp.where(same & (k == 0), 0.0, own)
        low = power(t1[0, i] + decode(ru[i]))
        high = power(t1[1, i] + decode(rd[i]))
        has_low, has_high = g > 0, g < s_ref[PLANES] - 1
        put_slot(outs, g ^ k, i, own.astype(jnp.bfloat16))
        put_slot(outs, jnp.where(has_low, (g - 1) ^ k, -1), i, low.astype(jnp.bfloat16))
        put_slot(outs, jnp.where(has_high, (g + 1) ^ k, -1), i, high.astype(jnp.bfloat16))
        sums[0:1, column_place(k, i, n)] = (
            column_total(own)
            + jnp.where(has_low, column_total(low), 0.0)
            + jnp.where(has_high, column_total(high), 0.0)
        )


def late_body(s_ref, t2, r2, rf, rn, before, *refs):
    outs, sums = refs[4:-1], refs[-1]
    k, g = s_ref[CHIP], s_ref[PLANE]
    n = t2.shape[-1]
    outer = (g == 0) | (g == s_ref[PLANES] - 1)
    for i in range(2):
        at = column_place(k, i, n)
        two = power(t2[0, i] + decode(r2[i]))
        three = power(decode(rf[i]) + decode(rn[i]))
        put_slot(outs, g ^ 2 ^ k, i, two.astype(jnp.bfloat16))
        put_slot(outs, jnp.where(outer, g ^ 3 ^ k, -1), i, three.astype(jnp.bfloat16))
        sums[0:1, at] = (
            before[0:1, at] + column_total(two) + jnp.where(outer, column_total(three), 0.0)
        )


def place_body(s_ref, t0, t1, t2, t3, out_ref):
    x = s_ref[SHIFT]
    tiles = (t0, t1, t2, t3)
    t = t0.shape[-1]
    for i in range(2):
        for c in range(4):
            v = tiles[c ^ i][i]
            for m in range(1, 4):
                v = jnp.where(x == m, tiles[c ^ i ^ m][i], v)
            out_ref[i * t : i * t + t, c * t : c * t + t] = v.astype(jnp.float32)


def pay_body(s_ref, a, *refs):
    a0, a1, b0, b1, out_n = refs[-5:]
    n, t = a.shape[0] // 2, a.shape[1] // 2
    a0[...] = a[:n, :t].T
    a1[...] = a[:n, t:].T
    b0[...] = a[n:, :t].T
    b1[...] = a[n:, t:].T
    first = pl.multiple_of(jnp.where(s_ref[PLANE] == 0, n, 0), n)
    out_n[...] = a[pl.ds(first, n)]


def hold_body(a, sums, out, chip):
    n = a.shape[0] // 2
    out[...] = a[...]
    wide = a[...].astype(jnp.float32)
    chip[0:1] = sums[0:1] + jnp.sum(wide[:n], axis=0, keepdims=True)
    chip[1:2] = sums[1:2] + jnp.sum(wide[n:], axis=0, keepdims=True)
    chip[2:3] = sums[2:3] + jnp.sum(wide * wide, axis=0, keepdims=True)


def limit(mib):
    return pltpu.CompilerParams(vmem_limit_bytes=mib * 1024 * 1024)


def whole():
    return pl.BlockSpec(memory_space=pltpu.VMEM)


def scalars():
    return pl.BlockSpec(memory_space=pltpu.SMEM)


def folded_shards(counts, library):
    rows, width = counts.shape
    n_cells = lax.axis_size("cells")
    n_genes = lax.axis_size("genes")
    cores = n_cells // n_genes
    total = float(rows * n_cells)
    half_cells = rows // 2
    half = width // cores
    tile = half // 2
    g = lax.axis_index("genes")
    c = lax.axis_index("cells")
    k, h = c // cores, c % cores

    def perm(f):
        pairs = []
        for ci in range(n_cells):
            for gi in range(n_genes):
                d = f(ci // cores, ci % cores, gi)
                if d is not None and 0 <= d[2] < n_genes:
                    pairs.append((ci * n_genes + gi, (d[0] * cores + d[1]) * n_genes + d[2]))
        return pairs

    def send(x, f):
        return lax.ppermute(x, AXES, perm(f))

    flip = lambda k, h, g: (k, h ^ 1, g)
    bf16, f32 = jnp.bfloat16, jnp.float32
    shape = jax.ShapeDtypeStruct

    last = n_genes - 1
    info = jnp.stack(
        [
            k,
            h,
            g,
            jnp.int32(n_genes),
            (g < n_genes // 2).astype(jnp.int32),
            jnp.where(g > 0, g ^ (g - 1), 0),
            jnp.where(g < last, g ^ (g + 1), 0),
            (2 * h) ^ k,
            (jnp.abs(k - g) <= 1).astype(jnp.int32),
        ]
    ).astype(jnp.int32)

    own = normalize(counts, library)
    oth = send(own, flip)
    pay_in = pl.BlockSpec((rows, half), lambda i, sc: (0, sc[CORE]))
    pay_shapes = [shape((tile, rows), bf16)] * 4 + [shape((rows, half), bf16)]

    def turn_payload(block, part, before):
        return pl.pallas_call(
            pay_body,
            grid_spec=pltpu.PrefetchScalarGridSpec(
                num_scalar_prefetch=1,
                grid=(1,),
                in_specs=[pay_in] + [pl.BlockSpec(memory_space=pl.ANY)] * len(before),
                out_specs=[pl.BlockSpec((tile, half_cells), lambda i, sc: (0, part))] * 4
                + [pl.BlockSpec((half_cells, half), lambda i, sc: (part, 0))],
            ),
            out_shape=pay_shapes,
            input_output_aliases={2 + n: n for n in range(len(before))},
            compiler_params=limit(8),
            name="turn_payload",
        )(info, block, *before)

    *pay, end = turn_payload(oth, 1, turn_payload(own, 0, []))
    up1 = [send(pay[i], lambda k, h, g: (k, h, g + 1)) for i in (0, 1)]
    dn1 = [send(pay[2 + i], lambda k, h, g: (k, h, g - 1)) for i in (0, 1)]
    widened = own.astype(f32)
    halves = jnp.sum(widened.reshape(2, half_cells, width), axis=1)
    squares = jnp.sum(widened * widened, axis=0)
    oth, chip = pl.pallas_call(
        hold_body,
        in_specs=[whole()] * 2,
        out_specs=[whole()] * 2,
        out_shape=[shape(oth.shape, bf16), shape((3, width), f32)],
        compiler_params=limit(14),
        name="hold",
    )(oth, jnp.concatenate([halves, squares[None]]))
    chip_halves = chip[:2]
    around = [send(chip, lambda k, h, g, j=j: (k ^ j, h, g)) for j in (1, 2, 3)]
    every = (chip + around[0]) + (around[1] + around[2])
    sums = [every[0] + every[1], every[2]]
    means = sums[0] / total
    variances = sums[1] / total - means * means
    packed = jnp.concatenate(
        [means[None], lax.rsqrt(variances + 1e-05)[None], chip_halves, jnp.zeros((4, width), f32)]
    )
    afar = [send(packed, lambda k, h, g, d=d: (k, h, g ^ d)) for d in (1, 2, 3)]
    own_stats = packed[None]
    stats = jnp.stack([packed] + afar)
    near = send(
        end, lambda k, h, g: (k, h, 1) if g == 0 else ((k, h, g - 1) if g == last else None)
    )

    def blocks(body, n, scratch, *operands, behind=0):
        return pl.pallas_call(
            functools.partial(body, total=total),
            in_specs=[scalars()]
            + [whole()] * (len(operands) - behind)
            + [pl.BlockSpec(memory_space=pl.ANY)] * behind,
            out_specs=[whole()] * 4,
            out_shape=[shape((n, 2, tile, tile), f32)]
            + [shape((n, 2, tile, tile), bf16)] * 3,
            scratch_shapes=[pltpu.VMEM(v, bf16) for v in scratch],
            compiler_params=limit(24),
            name="partial_blocks",
        )(info, *operands)

    up2 = [send(up1[i], lambda k, h, g: (k, h, g + 1) if g > 0 else None) for i in (0, 1)]
    dn2 = [send(dn1[i], lambda k, h, g: (k, h, g - 1) if g < last else None) for i in (0, 1)]
    near_other = send(near, flip)
    kept = (half, rows)
    w0 = blocks(diagonal_body, 1, [], *pay, own, oth, own_stats)
    w1 = blocks(near_body, 2, [], *up1, *dn1, own, oth, stats)
    w3 = blocks(ends_body, 1, [kept, (rows, width)], *up2, *dn2, near, near_other, stats)

    def reduce_tiles(w):
        return [w[0]] + [send(w[j], lambda k, h, g, j=j: (k ^ j, h, g)) for j in (1, 2, 3)]

    small = shape((2, tile, tile), bf16)

    def turn(parts, turns, keeps):
        n = parts[0].shape[0]
        n_out = sum(v is not None for v in turns + keeps)
        return pl.pallas_call(
            functools.partial(turn_body, turns=turns, keeps=keeps),
            in_specs=[scalars()] + [whole()] * 4,
            out_specs=[whole()] * (1 + n_out),
            out_shape=[shape((n, 2, tile, tile), f32)] + [small] * n_out,
            compiler_params=limit(12),
            name="sum_tiles",
        )(info, *parts)

    (t0,) = turn(reduce_tiles(w0), [None], [None])
    w2 = blocks(far_body, 1, [kept], *up2, *dn2, own, oth, stats)
    t1, e_up, e_dn = turn(reduce_tiles(w1), [0, 1], [None, None])
    t2, e_two = turn(reduce_tiles(w2), [0], [None])
    _, e_three, k_three = turn(reduce_tiles(w3), [0], [1])

    side = lambda f: (lambda k, h, g: (k, h ^ (k // 2), f(g)) if f(g) is not None else None)
    rd = send(e_up, side(lambda g: g - 1))
    ru = send(e_dn, side(lambda g: g + 1))
    r2 = send(e_two, side(lambda g: g ^ 2))
    inner = lambda g: 0 < g < last
    r3f = send(e_three, side(lambda g: (g ^ 2) if inner(g) else None))
    r3n = send(k_three, lambda k, h, g: (k, h, g ^ 1) if inner(g) else None)

    def finish(body, *operands, over=0):
        return pl.pallas_call(
            body,
            in_specs=[scalars()] + [whole()] * len(operands),
            input_output_aliases={1 + len(operands) - over + n: n for n in range(over)},
            out_specs=[whole()] * 5,
            out_shape=[small] * 4 + [shape((1, half), f32)],
            compiler_params=limit(10),
            name="finish_tiles",
        )(info, *operands)

    *close, close_sums = finish(early_body, t0, t1, ru, rd)
    *tiles, tile_sums = finish(late_body, t2, r2, r3f, r3n, close_sums, *close, over=len(close))
    got = [tiles[0]] + [send(tiles[j], lambda k, h, g, j=j: (k ^ j, h, g)) for j in (1, 2, 3)]
    adjacency = pl.pallas_call(
        place_body,
        in_specs=[scalars()] + [whole()] * 4,
        out_specs=whole(),
        out_shape=shape((half, width), f32),
        compiler_params=limit(12),
        name="place_tiles",
    )(info, *got)
    sums = [send(tile_sums, lambda k, h, g, m=m: (g, h ^ (k // 2), k ^ m)) for m in range(4)]
    connectivity = ((sums[0] + sums[1]) + (sums[2] + sums[3])).reshape(half)
    return (adjacency, connectivity)


def folded(counts, library):
    return folded_shards(counts, library)


def solution(mesh):
    cells, genes = mesh.shape["cells"], mesh.shape["genes"]
    folds = genes == 4 and cells == 2 * genes
    return jax.shard_map(
        folded if folds else general_shards,
        mesh=mesh,
        in_specs=(P("cells", "genes"), P("cells")),
        out_specs=(P("cells", "genes"), P("cells")),
        check_vma=False,
    )
```

```python
import functools

import jax
import jax.numpy as jnp
from jax import lax
from jax.experimental import pallas as pl
from jax.experimental.pallas import tpu as pltpu
from jax.sharding import PartitionSpec as P


AXES = ("cells", "genes")


def normalize(counts, library):
    factor = 10000.0 / library.astype(jnp.float32)
    return jnp.log1p(counts.astype(jnp.float32) * factor[:, None]).astype(jnp.bfloat16)


def cross_product(left, right):
    return lax.dot_general(
        left, right, (((0,), (0,)), ((), ())), preferred_element_type=jnp.float32
    )


def general_shards(counts, library):
    own_block = normalize(counts, library)
    col_width = own_block.shape[1]
    cell_groups = lax.axis_size("cells")
    gene_total = col_width * lax.axis_size("genes")
    row_width = gene_total // cell_groups
    total_cells = float(counts.shape[0] * cell_groups)
    widened = own_block.astype(jnp.float32)
    local_sums = jnp.sum(widened, axis=0)
    local_squares = jnp.sum(widened * widened, axis=0)
    block_sums, block_squares = lax.psum((local_sums, local_squares), "cells")
    gene_sums, gene_squares = (
        lax.all_gather(block_sums, "genes", axis=0, tiled=True),
        lax.all_gather(block_squares, "genes", axis=0, tiled=True),
    )
    full_block = lax.all_gather(own_block, "genes", axis=1, tiled=True)
    gram_tile = lax.psum_scatter(
        cross_product(full_block, own_block), "cells", scatter_dimension=0, tiled=True
    )
    means = gene_sums / total_cells
    variances = gene_squares / total_cells - means * means
    scales = lax.rsqrt(variances + 1e-05)
    row_first = lax.axis_index("cells") * row_width
    col_first = lax.axis_index("genes") * col_width
    row_means = lax.dynamic_slice_in_dim(means, row_first, row_width, 0)
    col_means = lax.dynamic_slice_in_dim(means, col_first, col_width, 0)
    row_scales = lax.dynamic_slice_in_dim(scales, row_first, row_width, 0)
    col_scales = lax.dynamic_slice_in_dim(scales, col_first, col_width, 0)
    correlation = (
        (gram_tile / total_cells - row_means[:, None] * col_means[None, :])
        * row_scales[:, None]
        * col_scales[None, :]
    )
    powered = correlation**6
    row_index = row_first + jnp.arange(row_width, dtype=jnp.int32)[:, None]
    col_index = col_first + jnp.arange(col_width, dtype=jnp.int32)[None, :]
    adjacency = jnp.where(row_index == col_index, jnp.float32(0.0), powered)
    connectivity = lax.psum(jnp.sum(adjacency, axis=1), "genes")
    return (adjacency, connectivity)


def encode(x):
    return (x * jnp.abs(x) * (x * x)).astype(jnp.bfloat16)


def decode(y):
    y = y.astype(jnp.float32)
    root = lax.rsqrt(lax.rsqrt(jnp.abs(y)))
    return jnp.where(y < 0, -root, root)


def plain(left, right):
    return jnp.dot(left, right, preferred_element_type=jnp.float32)


def put_tiles(product, sums, s_ref, blk, rst, cst, cells, total, outs):
    odd = s_ref[CHIP] % 2
    row_side = jnp.concatenate([rst, jnp.broadcast_to(sums(rst), rst.shape)]).T
    mr, sr = row_side[:, 0:1], row_side[:, 1:2] * (1.0 / total)
    sx = row_side[:, rst.shape[0] : rst.shape[0] + 1]
    half = sr.shape[0]
    t = half // 2
    base = s_ref[CORE] ^ (s_ref[CHIP] // 2)
    for jj in range(2):
        first = pl.multiple_of((base ^ jj) * half, half)
        stat = cst(first, half)
        mc, sc = stat[0:1], stat[1:2]
        rest = sums(stat) - cells * mc
        tiles = [[None, None], [None, None]]
        for c in range(2):
            lanes = slice(c * t, c * t + t)
            p = product(pl.multiple_of(first + c * t, t), t)
            p = (p - sx * mc[:, lanes] - mr * rest[:, lanes]) * sr * sc[:, lanes]
            tiles[0][c], tiles[1][c] = p[:t], p[t:]
        for b in range(2):
            for i in range(2):
                tile = jnp.where(odd == 0, tiles[i][i ^ b], tiles[i][1 - (i ^ b)])
                j = 2 * jj + b
                outs[j][blk, i] = encode(tile) if j else tile


def row_stats(s_ref, st, plane, half):
    return st[plane, :, pl.ds(pl.multiple_of(s_ref[CORE] * half, half), half)]


def column_stats(st, plane):
    return lambda first, n: st[plane, :, pl.ds(first, n)]


def stacked(products):
    return jnp.concatenate(products, axis=0)


def diagonal_body(s_ref, a0, a1, b0, b1, y0, y1, st, *outs, total):
    half = 2 * a0.shape[0]
    n = y0.shape[0] // 2

    def product(first, w):
        lanes = pl.ds(first, w)
        return stacked(
            [
                plain(xa[:, :n], y0[:n, lanes])
                + plain(xa[:, n:], y1[:n, lanes])
                + plain(xb[:, :n], y0[n:, lanes])
                + plain(xb[:, n:], y1[n:, lanes])
                for xa, xb in ((a0, b0), (a1, b1))
            ]
        )

    put_tiles(
        product, lambda v: v[2:3] + v[3:4], s_ref, 0,
        row_stats(s_ref, st, 0, half), column_stats(st, 0), 4.0 * n, total, outs,
    )


def near_body(s_ref, x0, x1, y0, y1, st, *outs, total, side):
    half = 2 * x0.shape[0]
    n = y0.shape[0] // 2
    cells = slice(side * n, side * n + n)

    def product(first, w):
        lanes = pl.ds(first, w)
        return stacked(
            [plain(x[:, :n], y0[cells, lanes]) + plain(x[:, n:], y1[cells, lanes]) for x in (x0, x1)]
        )

    put_tiles(
        product, lambda v: v[2 + side : 3 + side], s_ref, 0,
        row_stats(s_ref, st, s_ref[LOWER + side], half), column_stats(st, 0),
        2.0 * n, total, outs,
    )


def pick_far(s_ref, a0, a1, b0, b1, xs):
    t = a0.shape[0]

    @pl.when(s_ref[LOW] == 0)
    def _():
        xs[:t] = a0[...]
        xs[t:] = a1[...]

    @pl.when(s_ref[LOW] == 1)
    def _():
        xs[:t] = b0[...]
        xs[t:] = b1[...]


def put_far(s_ref, product, st, plane, outs, cells, half, total):
    put_tiles(
        product, lambda v: jnp.where(s_ref[LOW] == 0, v[2:3], v[3:4]), s_ref, 0,
        row_stats(s_ref, st, 2, half), column_stats(st, plane), cells, total, outs,
    )


def far_body(s_ref, a0, a1, b0, b1, y0, y1, st, *refs, total):
    xs, outs = refs[-1], refs[:-1]
    half = 2 * a0.shape[0]
    n = y0.shape[0] // 2
    pick_far(s_ref, a0, a1, b0, b1, xs)
    cells = pl.ds(pl.multiple_of(s_ref[LOW] * n, n), n)

    def product(first, w):
        lanes = pl.ds(first, w)
        return plain(xs[:, :n], y0[cells, lanes]) + plain(xs[:, n:], y1[cells, lanes])

    put_far(s_ref, product, st, 0, outs, 2.0 * n, half, total)


def ends_body(s_ref, a0, a1, b0, b1, na, nb, st, *refs, total):
    xs, ys, outs = refs[-2], refs[-1], refs[:-2]
    half = 2 * a0.shape[0]
    n = na.shape[0] // 2
    pick_far(s_ref, a0, a1, b0, b1, xs)

    @pl.when(s_ref[CORE] == 0)
    def _():
        ys[:, :half] = na[...]
        ys[:n, half:] = nb[n:]
        ys[n:, half:] = nb[:n]

    @pl.when(s_ref[CORE] == 1)
    def _():
        ys[:, half:] = na[...]
        ys[:n, :half] = nb[n:]
        ys[n:, :half] = nb[:n]

    put_far(
        s_ref, lambda first, w: plain(xs[...], ys[:, pl.ds(first, w)]), st, 1, outs,
        2.0 * n, half, total,
    )


CHIP, CORE, PLANE, PLANES, LOW, LOWER, _, SHIFT, _ = range(9)


def turn_body(s_ref, own, r1, r2, r3, *outs, turns, keeps):
    odd = s_ref[CHIP] % 2
    t_ref, rest = outs[0], outs[1:]
    for n in range(own.shape[0]):
        for i in range(2):
            v = own[n, i] + decode(r1[n, i]) + decode(r2[n, i]) + decode(r3[n, i])
            t_ref[n, i] = v
            if keeps[n] is not None:
                rest[keeps[n]][i] = encode(v)
            if turns[n] is not None:
                w = encode(v.T)
                dst = rest[turns[n]]

                @pl.when(odd == 0)
                def _():
                    dst[i] = w

                @pl.when(odd == 1)
                def _():
                    dst[1 - i] = w


def power(v):
    v2 = v * v
    return v2 * v2 * v2


def put_slot(outs, where, i, value):
    for j, o in enumerate(outs):

        @pl.when(where == j)
        def _():
            o[i] = value


def column_total(v):
    return jnp.sum(v, axis=0, keepdims=True)


def column_place(k, i, n):
    return pl.ds(pl.multiple_of((i ^ (k % 2)) * n, n), n)


def early_body(s_ref, t0, ta, tb, ru, rd, *refs):
    outs, sums = refs[:-1], refs[-1]
    k, g = s_ref[CHIP], s_ref[PLANE]
    n = t0.shape[-1]
    for i in range(2):
        own = power(t0[0, i])
        same = lax.broadcasted_iota(jnp.int32, (n, n), 0) == lax.broadcasted_iota(
            jnp.int32, (n, n), 1
        )
        own = jnp.where(same & (k == 0), 0.0, own)
        low = power(ta[0, i] + decode(ru[i]))
        high = power(tb[0, i] + decode(rd[i]))
        has_low, has_high = g > 0, g < s_ref[PLANES] - 1
        put_slot(outs, g ^ k, i, own.astype(jnp.bfloat16))
        put_slot(outs, jnp.where(has_low, (g - 1) ^ k, -1), i, low.astype(jnp.bfloat16))
        put_slot(outs, jnp.where(has_high, (g + 1) ^ k, -1), i, high.astype(jnp.bfloat16))
        sums[0:1, column_place(k, i, n)] = (
            column_total(own)
            + jnp.where(has_low, column_total(low), 0.0)
            + jnp.where(has_high, column_total(high), 0.0)
        )


def ends_finish_body(s_ref, rf, rn, before, *refs):
    outs, sums = refs[4:-1], refs[-1]
    k, g = s_ref[CHIP], s_ref[PLANE]
    n = rf.shape[-1]
    outer = (g == 0) | (g == s_ref[PLANES] - 1)
    for i in range(2):
        at = column_place(k, i, n)
        three = power(decode(rf[i]) + decode(rn[i]))
        put_slot(outs, jnp.where(outer, g ^ 3 ^ k, -1), i, three.astype(jnp.bfloat16))
        sums[0:1, at] = before[0:1, at] + jnp.where(outer, column_total(three), 0.0)


def late_body(s_ref, t2, r2, before, *refs):
    outs, sums = refs[4:-1], refs[-1]
    k, g = s_ref[CHIP], s_ref[PLANE]
    n = t2.shape[-1]
    for i in range(2):
        at = column_place(k, i, n)
        two = power(t2[0, i] + decode(r2[i]))
        put_slot(outs, g ^ 2 ^ k, i, two.astype(jnp.bfloat16))
        sums[0:1, at] = before[0:1, at] + column_total(two)


def place_body(s_ref, t0, t1, t2, t3, out_ref):
    x = s_ref[SHIFT]
    tiles = (t0, t1, t2, t3)
    t = t0.shape[-1]
    for i in range(2):
        for c in range(4):
            v = tiles[c ^ i][i]
            for m in range(1, 4):
                v = jnp.where(x == m, tiles[c ^ i ^ m][i], v)
            out_ref[i * t : i * t + t, c * t : c * t + t] = v.astype(jnp.float32)


def pay_body(s_ref, a, *refs):
    a0, a1, b0, b1, out_n = refs[-5:]
    n, t = a.shape[0] // 2, a.shape[1] // 2
    a0[...] = a[:n, :t].T
    a1[...] = a[:n, t:].T
    b0[...] = a[n:, :t].T
    b1[...] = a[n:, t:].T
    first = pl.multiple_of(jnp.where(s_ref[PLANE] == 0, n, 0), n)
    out_n[...] = a[pl.ds(first, n)]


def hold_body(a, sums, out, chip):
    n = a.shape[0] // 2
    out[...] = a[...]
    wide = a[...].astype(jnp.float32)
    chip[0:1] = sums[0:1] + jnp.sum(wide[:n], axis=0, keepdims=True)
    chip[1:2] = sums[1:2] + jnp.sum(wide[n:], axis=0, keepdims=True)
    chip[2:3] = sums[2:3] + jnp.sum(wide * wide, axis=0, keepdims=True)


def limit(mib):
    return pltpu.CompilerParams(vmem_limit_bytes=mib * 1024 * 1024)


def whole():
    return pl.BlockSpec(memory_space=pltpu.VMEM)


def scalars():
    return pl.BlockSpec(memory_space=pltpu.SMEM)


def folded_shards(counts, library):
    rows, width = counts.shape
    n_cells = lax.axis_size("cells")
    n_genes = lax.axis_size("genes")
    cores = n_cells // n_genes
    total = float(rows * n_cells)
    half_cells = rows // 2
    half = width // cores
    tile = half // 2
    g = lax.axis_index("genes")
    c = lax.axis_index("cells")
    k, h = c // cores, c % cores

    def perm(f):
        pairs = []
        for ci in range(n_cells):
            for gi in range(n_genes):
                d = f(ci // cores, ci % cores, gi)
                if d is not None and 0 <= d[2] < n_genes:
                    pairs.append((ci * n_genes + gi, (d[0] * cores + d[1]) * n_genes + d[2]))
        return pairs

    def send(x, f):
        return lax.ppermute(x, AXES, perm(f))

    flip = lambda k, h, g: (k, h ^ 1, g)
    bf16, f32 = jnp.bfloat16, jnp.float32
    shape = jax.ShapeDtypeStruct

    last = n_genes - 1
    info = jnp.stack(
        [
            k,
            h,
            g,
            jnp.int32(n_genes),
            (g < n_genes // 2).astype(jnp.int32),
            jnp.where(g > 0, g ^ (g - 1), 0),
            jnp.where(g < last, g ^ (g + 1), 0),
            (2 * h) ^ k,
            (jnp.abs(k - g) <= 1).astype(jnp.int32),
        ]
    ).astype(jnp.int32)

    own = normalize(counts, library)
    oth = send(own, flip)
    pay_in = pl.BlockSpec((rows, half), lambda i, sc: (0, sc[CORE]))
    pay_shapes = [shape((tile, rows), bf16)] * 4 + [shape((rows, half), bf16)]

    def turn_payload(block, part, before):
        return pl.pallas_call(
            pay_body,
            grid_spec=pltpu.PrefetchScalarGridSpec(
                num_scalar_prefetch=1,
                grid=(1,),
                in_specs=[pay_in] + [pl.BlockSpec(memory_space=pl.ANY)] * len(before),
                out_specs=[pl.BlockSpec((tile, half_cells), lambda i, sc: (0, part))] * 4
                + [pl.BlockSpec((half_cells, half), lambda i, sc: (part, 0))],
            ),
            out_shape=pay_shapes,
            input_output_aliases={2 + n: n for n in range(len(before))},
            compiler_params=limit(8),
            name="turn_payload",
        )(info, block, *before)

    *pay, end = turn_payload(oth, 1, turn_payload(own, 0, []))
    up1 = [send(pay[i], lambda k, h, g: (k, h, g + 1)) for i in (0, 1)]
    dn1 = [send(pay[2 + i], lambda k, h, g: (k, h, g - 1)) for i in (0, 1)]
    widened = own.astype(f32)
    halves = jnp.sum(widened.reshape(2, half_cells, width), axis=1)
    squares = jnp.sum(widened * widened, axis=0)
    oth, chip = pl.pallas_call(
        hold_body,
        in_specs=[whole()] * 2,
        out_specs=[whole()] * 2,
        out_shape=[shape(oth.shape, bf16), shape((3, width), f32)],
        compiler_params=limit(14),
        name="hold",
    )(oth, jnp.concatenate([halves, squares[None]]))
    chip_halves = chip[:2]
    around = [send(chip, lambda k, h, g, j=j: (k ^ j, h, g)) for j in (1, 2, 3)]
    every = (chip + around[0]) + (around[1] + around[2])
    sums = [every[0] + every[1], every[2]]
    means = sums[0] / total
    variances = sums[1] / total - means * means
    packed = jnp.concatenate(
        [means[None], lax.rsqrt(variances + 1e-05)[None], chip_halves, jnp.zeros((4, width), f32)]
    )
    afar = [send(packed, lambda k, h, g, d=d: (k, h, g ^ d)) for d in (1, 2, 3)]
    own_stats = packed[None]
    stats = jnp.stack([packed] + afar)
    near = send(
        end, lambda k, h, g: (k, h, 1) if g == 0 else ((k, h, g - 1) if g == last else None)
    )

    def blocks(body, n, scratch, *operands, behind=0, **extra):
        return pl.pallas_call(
            functools.partial(body, total=total, **extra),
            in_specs=[scalars()]
            + [whole()] * (len(operands) - behind)
            + [pl.BlockSpec(memory_space=pl.ANY)] * behind,
            out_specs=[whole()] * 4,
            out_shape=[shape((n, 2, tile, tile), f32)]
            + [shape((n, 2, tile, tile), bf16)] * 3,
            scratch_shapes=[pltpu.VMEM(v, bf16) for v in scratch],
            compiler_params=limit(24),
            name="partial_blocks",
        )(info, *operands)

    up2 = [send(up1[i], lambda k, h, g: (k, h, g + 1) if g > 0 else None) for i in (0, 1)]
    dn2 = [send(dn1[i], lambda k, h, g: (k, h, g - 1) if g < last else None) for i in (0, 1)]
    near_other = send(near, flip)
    kept = (half, rows)
    w0 = blocks(diagonal_body, 1, [], *pay, own, oth, own_stats)
    w1a = blocks(near_body, 1, [], *up1, own, oth, stats, side=0)
    w1b = blocks(near_body, 1, [], *dn1, own, oth, stats, side=1)
    w3 = blocks(ends_body, 1, [kept, (rows, width)], *up2, *dn2, near, near_other, stats)

    def reduce_tiles(w):
        return [w[0]] + [send(w[j], lambda k, h, g, j=j: (k ^ j, h, g)) for j in (1, 2, 3)]

    small = shape((2, tile, tile), bf16)

    def turn(parts, turns, keeps):
        n = parts[0].shape[0]
        n_out = sum(v is not None for v in turns + keeps)
        return pl.pallas_call(
            functools.partial(turn_body, turns=turns, keeps=keeps),
            in_specs=[scalars()] + [whole()] * 4,
            out_specs=[whole()] * (1 + n_out),
            out_shape=[shape((n, 2, tile, tile), f32)] + [small] * n_out,
            compiler_params=limit(12),
            name="sum_tiles",
        )(info, *parts)

    (t0,) = turn(reduce_tiles(w0), [None], [None])
    w2 = blocks(far_body, 1, [kept], *up2, *dn2, own, oth, stats)
    ta, e_up = turn(reduce_tiles(w1a), [0], [None])
    tb, e_dn = turn(reduce_tiles(w1b), [0], [None])
    t2, e_two = turn(reduce_tiles(w2), [0], [None])
    _, e_three, k_three = turn(reduce_tiles(w3), [0], [1])

    side = lambda f: (lambda k, h, g: (k, h ^ (k // 2), f(g)) if f(g) is not None else None)
    rd = send(e_up, side(lambda g: g - 1))
    ru = send(e_dn, side(lambda g: g + 1))
    r2 = send(e_two, side(lambda g: g ^ 2))
    inner = lambda g: 0 < g < last
    r3f = send(e_three, side(lambda g: (g ^ 2) if inner(g) else None))
    r3n = send(k_three, lambda k, h, g: (k, h, g ^ 1))

    def finish(body, *operands, over=0):
        return pl.pallas_call(
            body,
            in_specs=[scalars()] + [whole()] * len(operands),
            input_output_aliases={1 + len(operands) - over + n: n for n in range(over)},
            out_specs=[whole()] * 5,
            out_shape=[small] * 4 + [shape((1, half), f32)],
            compiler_params=limit(10),
            name="finish_tiles",
        )(info, *operands)

    *close, close_sums = finish(early_body, t0, ta, tb, ru, rd)
    *most, most_sums = finish(ends_finish_body, r3f, r3n, close_sums, *close, over=len(close))
    *tiles, tile_sums = finish(late_body, t2, r2, most_sums, *most, over=len(most))
    got = [tiles[0]] + [send(tiles[j], lambda k, h, g, j=j: (k ^ j, h, g)) for j in (1, 2, 3)]
    adjacency = pl.pallas_call(
        place_body,
        in_specs=[scalars()] + [whole()] * 4,
        out_specs=whole(),
        out_shape=shape((half, width), f32),
        compiler_params=limit(12),
        name="place_tiles",
    )(info, *got)
    sums = [send(tile_sums, lambda k, h, g, m=m: (g, h ^ (k // 2), k ^ m)) for m in range(4)]
    connectivity = ((sums[0] + sums[1]) + (sums[2] + sums[3])).reshape(half)
    return (adjacency, connectivity)


def folded(counts, library):
    return folded_shards(counts, library)


def solution(mesh):
    cells, genes = mesh.shape["cells"], mesh.shape["genes"]
    folds = genes == 4 and cells == 2 * genes
    return jax.shard_map(
        folded if folds else general_shards,
        mesh=mesh,
        in_specs=(P("cells", "genes"), P("cells")),
        out_specs=(P("cells", "genes"), P("cells")),
        check_vma=False,
    )
```
